128 devices in a mesh: dp: 2 (over z_hi), row: 4 (over x), col: 16 (over z_lo, y, core).
Axes of the slice: x: 4, y: 4, z: 4 (z_hi: 2, z_lo: 2; z = z_hi * 2 + z_lo), core: 2. Of those that a mesh axis runs over, the one named last changes fastest.
Arguments:
- stash_codes: int32 [4096, 4096], P(('dp', 'col'), 'row'), may hold values from 0 to 3
- stash_scales: int32 [4096, 32], P(('dp', 'col'), 'row'), may hold values from 1 to 8
- pad_mask: int32 [4096], P(('dp', 'col')), may hold values 0 or 1
- cotangent: bfloat16 [4096, 4096], P(('dp', 'col'), 'row'), may hold values from -3 to 3
- w_gate: bfloat16 [4096, 10240], P('row', 'col'), may hold values from -0.09375 to 0.09375
- w_up: bfloat16 [4096, 10240], P('row', 'col'), may hold values from -0.09375 to 0.09375
- w_out: bfloat16 [4096, 10240], P('row', 'col'), may hold values from -0.09375 to 0.09375
Outputs:
- input_grad: float32 [4096, 4096], P(('dp', 'col'), 'row')
- gate_weight_grad: float32 [4096, 10240], P('row', 'col')
- up_weight_grad: float32 [4096, 10240], P('row', 'col')
- out_weight_grad: float32 [4096, 10240], P('row', 'col')
The draws below stay inside these ranges and needn't reach their ends.
All inputs are finite; a program needn't handle non-finite values. No bound on the sum of `pad_mask` on one device may be relied on, other than what follows from the above.
Results may differ from the reference program's by a relative error of at most 0.0029.
Values may be sent and summed in bfloat16 or wider, within the bound.
A program may use at most 128 MiB of HBM per device.

```python
import jax
import jax.numpy as jnp

D = 4096
FF = 10240
QBLOCK = 128
TOKENS = 4096


def place_ends(result, stream_key, least, high):
    longest = result.shape.index(max(result.shape))
    spots = []
    for shift in (0, 1):
        where = [jax.random.randint(jax.random.fold_in(stream_key, axis), (), 0, length) for axis, length in enumerate(result.shape)]
        where[longest] = (where[longest] + shift) % result.shape[longest]
        spots.append(tuple(where))
    return result.at[spots[0]].set(least).at[spots[1]].set(high)


def level_of(own_key, dims, split, least, top_value):
    factor_of, own = 1.0, jax.random.fold_in(own_key, 6)
    for axis_at, blocks in split:
        draws = jnp.exp(jax.random.uniform(jax.random.fold_in(own, axis_at), (blocks,), jnp.float32, least / len(split), top_value / len(split)))
        factor_of = factor_of * jnp.repeat(draws, dims[axis_at] // blocks).reshape([-1 if axis == axis_at else 1 for axis in range(len(dims))])
    return factor_of


def scatter_about(stream_key, extent, scale, most, cuts=(), kind=jnp.bfloat16):
    entries = jax.random.normal(stream_key, extent, jnp.float32) * scale
    if len(cuts) > 0:
        entries = level_of(stream_key, extent, cuts, -0.22, 0.18) * entries
    return jnp.clip(entries, min=-most, max=most).astype(kind)


def setup_inputs(seed: int = 0) -> dict:
    streams_of = jax.random.split(jax.random.key(seed), 8)
    stash_codes = place_ends(jax.random.randint(streams_of[0], (TOKENS, D), 0, 4), jax.random.fold_in(streams_of[0], 1), 0, 3).astype(jnp.int32)
    stash_scales = place_ends(jax.random.randint(streams_of[1], (TOKENS, D // QBLOCK), 1, 9), jax.random.fold_in(streams_of[1], 1), 1, 8).astype(jnp.int32)
    pad_mask = place_ends((jax.random.randint(streams_of[2], (TOKENS,), 0, 4) < 3).astype(jnp.int32), jax.random.fold_in(streams_of[2], 1), 0, 1)
    cotangent = scatter_about(streams_of[3], (TOKENS, D), 0.5, 3.0, ((0, 32), (1, 4)))
    w_gate = scatter_about(streams_of[4], (D, FF), D ** -0.5, 0.09375, ((0, 4), (1, 16)))
    w_up = scatter_about(streams_of[5], (D, FF), D ** -0.5, 0.09375, ((0, 4), (1, 16)))
    w_out = scatter_about(streams_of[6], (D, FF), D ** -0.5, 0.09375, ((0, 4), (1, 16)))
    return dict(stash_codes=stash_codes, stash_scales=stash_scales, pad_mask=pad_mask, cotangent=cotangent, w_gate=w_gate, w_up=w_up, w_out=w_out)


root_term = 0.7978845608028654
cubic_term = 0.044715


def gelu_pair(values):
    inside = root_term * (values + cubic_term * values * values * values)
    tangent = jnp.tanh(inside)
    activated = 0.5 * values * (1.0 + tangent)
    derivative = 0.5 * (1.0 + tangent) + 0.5 * values * (1.0 - tangent * tangent) * root_term * (1.0 + 3.0 * cubic_term * values * values)
    return activated, derivative


def unpack_stash(stash_codes, stash_scales):
    blocks = stash_scales.shape[1]
    block_width = stash_codes.shape[1] // blocks
    levels = (2 * stash_codes - 3).astype(jnp.float32).reshape(stash_codes.shape[0], blocks, block_width)
    scaled = levels * stash_scales.astype(jnp.float32)[:, :, None] / 16.0
    return scaled.reshape(stash_codes.shape).astype(jnp.bfloat16)


def reference(stash_codes, stash_scales, pad_mask, cotangent, w_gate, w_up, w_out):
    stashed = unpack_stash(stash_codes, stash_scales)
    live_grad = (cotangent.astype(jnp.float32) * pad_mask.astype(jnp.float32)[:, None]).astype(jnp.bfloat16)
    gate_pre = jnp.dot(stashed, w_gate, preferred_element_type=jnp.float32)
    up_part = jnp.dot(stashed, w_up, preferred_element_type=jnp.float32)
    back_grad = jnp.dot(live_grad, w_out, preferred_element_type=jnp.float32)
    activated, derivative = gelu_pair(gate_pre)
    hidden = (activated * up_part).astype(jnp.bfloat16)
    gate_grad = (back_grad * up_part * derivative).astype(jnp.bfloat16)
    up_grad = (back_grad * activated).astype(jnp.bfloat16)
    input_grad = jnp.dot(gate_grad, w_gate.T, preferred_element_type=jnp.float32) + jnp.dot(up_grad, w_up.T, preferred_element_type=jnp.float32)
    gate_weight_grad = jnp.dot(stashed.T, gate_grad, preferred_element_type=jnp.float32)
    up_weight_grad = jnp.dot(stashed.T, up_grad, preferred_element_type=jnp.float32)
    out_weight_grad = jnp.dot(live_grad.T, hidden, preferred_element_type=jnp.float32)
    return input_grad, gate_weight_grad, up_weight_grad, out_weight_grad
```

```python
import functools

import jax
import jax.numpy as jnp
from jax import lax
from jax.experimental import pallas as pl
from jax.experimental.pallas import tpu as pltpu
from jax.sharding import PartitionSpec as P

MESH = pl.DeviceIdType.MESH
ROOT = 0.7978845608028654
CUBIC = 0.044715
W = 128
FOOT = 16
F32 = jnp.float32
BF16 = jnp.bfloat16


def gelu_pair(values):
    inside = ROOT * (values + CUBIC * values * values * values)
    tangent = jnp.tanh(inside)
    activated = 0.5 * values * (1.0 + tangent)
    derivative = 0.5 * (1.0 + tangent) + 0.5 * values * (1.0 - tangent * tangent) * ROOT * (
        1.0 + 3.0 * CUBIC * values * values
    )
    return activated, derivative


def coded(part):
    most = jnp.maximum(jnp.max(jnp.abs(part), axis=0, keepdims=True), 1e-30)
    power = jnp.floor(jnp.log(most) * 1.4426950408889634) + 1.0
    units = jnp.round(part * jnp.exp2(15.0 - power))
    units = jnp.clip(units, -32767.0, 32767.0).astype(jnp.int32).astype(jnp.int16)
    foot = jnp.broadcast_to(power, (FOOT, part.shape[1])).astype(jnp.int32).astype(jnp.int16)
    return units, foot


def store_coded(tile, lanes, part):
    rows = part.shape[0]
    units, foot = coded(part)
    tile[pl.ds(0, rows), lanes] = units
    tile[pl.ds(rows, FOOT), lanes] = foot


def decoded(tile, rows, lanes):
    power = tile[pl.ds(rows, FOOT), lanes].astype(jnp.int32).astype(F32)[0:1]
    units = tile[pl.ds(0, rows), lanes].astype(jnp.int32).astype(F32)
    return units * jnp.exp2(power - 15.0)


def kernel(
    dims,
    codes, scales, mask, cot, wg, wu, wo,
    dx_out, g_out, u_out, o_out,
    sl, wc, pb, r1, r2, guh, dx, dws, dwr, stage, dxs, dxr, dfr,
    w_sem, ag_s, ag_r, rs1_s, rs1_r, rs2_s, rs2_r, a1_s, a1_r, a2_s, a2_r,
    dp_s, dp_r, out_sem, dxc_s, dxc_r, dx_s, dx_r,
):
    tb, dl, chunks = dims
    blk = 4 * tb
    half = 2 * tb
    x = lax.axis_index("row")
    col = lax.axis_index("col")
    dp = lax.axis_index("dp")
    core = lax.rem(col, 2)
    y = lax.rem(col // 2, 4)
    z = col // 8
    right, left, opp = lax.rem(x + 1, 4), lax.rem(x + 3, 4), lax.rem(x + 2, 4)

    def at_col(dz, dy, dc):
        zz = (1 - z) if dz else z
        cc = (1 - core) if dc else core
        return {"col": (zz * 4 + lax.rem(y + dy, 4)) * 2 + cc}

    to_right, to_left, to_dp = {"row": right}, {"row": left}, {"dp": 1 - dp}
    STEP = (0, 3, 1, 2)
    others = [(b, zr) for b in range(4) for zr in range(2) if (b, zr) != (0, 0)]

    barrier = pltpu.get_barrier_semaphore()
    peers = [to_right, to_left, to_dp, at_col(0, 0, 1)]
    peers += [at_col(zr, STEP[b], 0) for b, zr in others]
    for peer in peers:
        pl.semaphore_signal(barrier, inc=1, device_id=peer, device_id_type=MESH)

    def weight_copy(j, m, src):
        return pltpu.make_async_copy(
            src.at[:, pl.ds(j * W, W)], wc.at[j, :, pl.ds(m * W, W)], w_sem.at[j, m]
        )

    for j in range(chunks):
        for m, src in enumerate((wg, wu, wo)):
            weight_copy(j, m, src).start()

    for k in range(dl // 128):
        lanes = pl.ds(k * 128, 128)
        level = (2 * codes[:, lanes] - 3) * scales[:, k : k + 1]
        sl[pl.ds(0, tb), lanes] = (level.astype(F32) * 0.0625).astype(BF16)
        live = cot[:, lanes].astype(F32) * mask[...].astype(F32)
        sl[pl.ds(0, tb), pl.ds(dl + k * 128, 128)] = live.astype(BF16)

    pl.semaphore_wait(barrier, len(peers))

    def remote(src, dst, s_sem, r_sem, device):
        return pltpu.make_async_remote_copy(
            src_ref=src, dst_ref=dst, send_sem=s_sem, recv_sem=r_sem,
            device_id=device, device_id_type=MESH,
        )

    def slot(b, zr, cr):
        return (b * 4 + zr * 2 + cr) * tb

    def rows(start, count):
        return sl.at[pl.ds(start, count)]

    started = []

    def gather(kind, src, dst, count, device):
        copy = remote(rows(src, count), rows(dst, count), ag_s.at[kind], ag_r.at[kind], device)
        copy.start()
        started.append(copy)

    def arrived(kind, dst, count):
        remote(
            rows(dst, count), rows(dst, count), ag_s.at[kind], ag_r.at[kind], at_col(0, 0, 1)
        ).wait_recv()

    def to_core(kind, b, zr):
        gather(9 + kind, slot(b, zr, 0), slot(b, zr, 1), tb, at_col(0, 0, 1))

    up, down = at_col(0, 1, 0), at_col(0, 3, 0)
    part = tb // 2
    gather(0, slot(0, 0, 0), slot(0, 1, 0), tb, at_col(1, 0, 0))
    gather(1, slot(0, 0, 0), slot(1, 0, 0), tb, up)
    gather(2, slot(0, 0, 0), slot(2, 0, 0), tb, down)
    to_core(0, 0, 0)
    for j in range(chunks):
        for m, src in enumerate((wg, wu, wo)):
            weight_copy(j, m, src).wait()

    def forward(j, b):
        into = pb.at[lax.rem(j, 3)]
        for h in range(2):
            where = pl.ds(pl.multiple_of(b * blk + h * half, half), half)
            tile = into.at[b, h]
            both = jnp.dot(
                sl[where, pl.ds(0, dl)], wc[j, :, pl.ds(0, 2 * W)], preferred_element_type=F32
            )
            store_coded(tile, pl.ds(0, 2 * W), both)
            back = jnp.dot(
                sl[where, pl.ds(dl, dl)], wc[j, :, pl.ds(2 * W, W)], preferred_element_type=F32
            )
            store_coded(tile, pl.ds(2 * W, W), back)

    def rs1(j, way):
        into = pb.at[lax.rem(j, 3)]
        return remote(
            into.at[opp, way], r1.at[j, way], rs1_s.at[j, way], rs1_r.at[j, way],
            (to_right, to_left)[way],
        )

    def rs2(j, way):
        into = pb.at[lax.rem(j, 3)]
        return remote(
            into.at[(right, left)[way]], r2.at[j, way], rs2_s.at[j, way], rs2_r.at[j, way],
            (to_right, to_left)[way],
        )

    def block_rows(j, b):
        return guh.at[j, pl.ds(pl.multiple_of(b * blk, blk), blk)]

    def half_rows(j, b, h):
        return guh.at[j, pl.ds(pl.multiple_of(b * blk + h * half, half), half)]

    def a1(j, way):
        return remote(
            block_rows(j, x), block_rows(j, x), a1_s.at[j, way], a1_r.at[j, way],
            (to_right, to_left)[way],
        )

    def a1_arrival(j, way):
        from_block = (left, right)[way]
        return remote(
            block_rows(j, from_block), block_rows(j, from_block), a1_s.at[j, way],
            a1_r.at[j, way], (to_right, to_left)[way],
        )

    def a2(j, way):
        b = (left, right)[way]
        return remote(
            half_rows(j, b, way), half_rows(j, b, way), a2_s.at[j, way], a2_r.at[j, way],
            (to_right, to_left)[way],
        )

    def a2_arrival(j, way):
        return remote(
            half_rows(j, opp, way), half_rows(j, opp, way), a2_s.at[j, way], a2_r.at[j, way],
            (to_right, to_left)[way],
        )

    def send_rs1(j):
        for way in range(2):
            rs1(j, way).start()

    def stage_f(j):
        def body(b, carry):
            forward(j, b)
            return carry

        lax.fori_loop(0, 4, body, 0)
        send_rs1(j)

    def stage_r(j):
        into = pb.at[lax.rem(j, 3)]
        for way in range(2):
            rs1(j, way).wait_recv()
            tile = into.at[(right, left)[way], way]
            for m in range(3):
                lanes = pl.ds(m * W, W)
                total = decoded(tile, half, lanes) + decoded(r1.at[j, way], half, lanes)
                store_coded(tile, lanes, total)
            rs2(j, way).start()

    def stage_a(j):
        into = pb.at[lax.rem(j, 3)]
        for way in range(2):
            rs2(j, way).wait_recv()
        for h in range(2):
            powers = []
            for m in range(3):
                lanes = pl.ds(m * W, W)
                powers.append(
                    [
                        jnp.exp2(
                            t[pl.ds(half, FOOT), lanes].astype(jnp.int32).astype(F32)[0:1] - 15.0
                        )
                        for t in (into.at[x, h], r2.at[j, 0, h], r2.at[j, 1, h])
                    ]
                )

            def body(k, carry, h=h, powers=powers):
                some = pl.ds(pl.multiple_of(k * 64, 64), 64)
                sums = []
                for m in range(3):
                    lanes = pl.ds(m * W, W)
                    total = None
                    for t, power in zip((into.at[x, h], r2.at[j, 0, h], r2.at[j, 1, h]), powers[m]):
                        term = t[some, lanes].astype(jnp.int32).astype(F32) * power
                        total = term if total is None else total + term
                    sums.append(total)
                gate, up_part, back = sums
                activated, derivative = gelu_pair(gate)
                to = pl.ds(pl.multiple_of(x * blk + h * half + k * 64, 64), 64)
                guh[j, to, pl.ds(0, W)] = (back * up_part * derivative).astype(BF16)
                guh[j, to, pl.ds(W, W)] = (back * activated).astype(BF16)
                guh[j, to, pl.ds(2 * W, W)] = (activated * up_part).astype(BF16)
                return carry

            lax.fori_loop(0, half // 64, body, 0)
        for way in range(2):
            a1(j, way).start()
        for way in range(2):
            rs1(j, way).wait_send()
            rs2(j, way).wait_send()

    def stage_w(j):
        for way in range(2):
            a1_arrival(j, way).wait_recv()
            a2(j, way).start()

    def dp_copy(j):
        return remote(dws.at[j], dwr.at[j], dp_s.at[j], dp_r.at[j], to_dp)

    def stage_dx(j):
        for way in range(2):
            a2_arrival(j, way).wait_recv()

        def body(k, carry):
            where = pl.ds(pl.multiple_of(k * half, half), half)
            more = lax.dot_general(
                guh[j, where, pl.ds(0, 2 * W)], wc[j, :, pl.ds(0, 2 * W)],
                (((1,), (1,)), ((), ())), preferred_element_type=F32,
            )
            dx[where, :] = dx[where, :] + more
            return carry

        lax.fori_loop(0, 8, body, 0)

    def stage_dw(j):
        def body(k, carry):
            where = pl.ds(pl.multiple_of(k * 256, 256), 256)
            some = lax.dot_general(
                sl[:, where], guh[j, :, pl.ds(0, 2 * W)],
                (((0,), (0,)), ((), ())), preferred_element_type=F32,
            )
            dws[j, where, pl.ds(0, 2 * W)] = some.astype(BF16)
            last = lax.dot_general(
                sl[:, pl.ds(pl.multiple_of(dl + k * 256, 256), 256)], guh[j, :, pl.ds(2 * W, W)],
                (((0,), (0,)), ((), ())), preferred_element_type=F32,
            )
            dws[j, where, pl.ds(2 * W, W)] = last.astype(BF16)
            return carry

        lax.fori_loop(0, dl // 256, body, 0)
        dp_copy(j).start()

    def out_copy(j, m):
        return pltpu.make_async_copy(
            stage.at[lax.rem(j, 2), m],
            (g_out, u_out, o_out)[m].at[:, pl.ds(pl.multiple_of(j * W, W), W)],
            out_sem.at[j, m],
        )

    def stage_e(j):
        dp_copy(j).wait()

        @pl.when(j >= 2)
        def _():
            for m in range(3):
                out_copy(j - 2, m).wait()

        def body(k, carry):
            where = pl.ds(pl.multiple_of(k * 128, 128), 128)
            for m in range(3):
                lanes = pl.ds(m * W, W)
                stage[lax.rem(j, 2), m, where, :] = dws[j, where, lanes].astype(F32) + dwr[
                    j, where, lanes
                ].astype(F32)
            return carry

        lax.fori_loop(0, dl // 128, body, 0)
        for m in range(3):
            out_copy(j, m).start()

    arrived(0, slot(0, 1, 0), tb)
    gather(3, slot(0, 1, 0), slot(1, 1, 0), tb, up)
    gather(4, slot(0, 1, 0), slot(2, 1, 0), tb, down)
    to_core(1, 0, 1)
    arrived(1, slot(1, 0, 0), tb)
    gather(5, slot(1, 0, 0), slot(3, 0, 0), part, up)
    to_core(2, 1, 0)
    arrived(2, slot(2, 0, 0), tb)
    gather(6, slot(2, 0, 0) + part, slot(3, 0, 0) + part, part, down)
    to_core(3, 2, 0)
    arrived(9, slot(0, 0, 1), tb)
    arrived(10, slot(0, 1, 1), tb)
    forward(0, 0)
    arrived(3, slot(1, 1, 0), tb)
    gather(7, slot(1, 1, 0), slot(3, 1, 0), part, up)
    to_core(4, 1, 1)
    arrived(4, slot(2, 1, 0), tb)
    gather(8, slot(2, 1, 0) + part, slot(3, 1, 0) + part, part, down)
    to_core(5, 2, 1)
    arrived(11, slot(1, 0, 1), tb)
    arrived(13, slot(1, 1, 1), tb)
    forward(0, 1)
    arrived(12, slot(2, 0, 1), tb)
    arrived(14, slot(2, 1, 1), tb)
    forward(0, 2)
    arrived(5, slot(3, 0, 0), part)
    arrived(6, slot(3, 0, 0) + part, part)
    to_core(6, 3, 0)
    arrived(7, slot(3, 1, 0), part)
    arrived(8, slot(3, 1, 0) + part, part)
    to_core(7, 3, 1)
    arrived(15, slot(3, 0, 1), tb)
    arrived(16, slot(3, 1, 1), tb)
    forward(0, 3)
    send_rs1(0)
    dx[...] = jnp.zeros_like(dx)

    def step(t, carry):
        def at(lag, fn, least=0):
            @pl.when(jnp.logical_and(t - lag >= least, t - lag < chunks))
            def _():
                fn(t - lag)

        at(0, stage_f, 1)
        at(1, stage_r)
        at(2, stage_a)
        at(3, stage_w)
        at(4, stage_dx)
        at(4, stage_dw)
        at(6, stage_e)
        return carry

    lax.fori_loop(0, chunks + 4, step, 0)

    core_copy = remote(dxs, dxr, dxc_s.at[0], dxc_r.at[0], at_col(0, 0, 1))
    for i in range(8):
        dxs[i] = dx[pl.ds((2 * i + 1) * tb, tb), :].astype(BF16)
    core_copy.start()
    for j in range(chunks - 2, chunks - 1):
        stage_e(j)
    core_copy.wait()

    def chip_copy(i):
        b, zr = i // 2, i % 2
        return remote(
            dxs.at[i], dfr.at[i], dx_s.at[i], dx_r.at[i], at_col(zr, STEP[b], 0)
        )

    for i in range(1, 8):
        total = dx[pl.ds(2 * i * tb, tb), :] + dxr[i].astype(F32)
        dxs[i] = total.astype(BF16)
        chip_copy(i).start()
    stage_e(chunks - 1)
    total = dx[pl.ds(0, tb), :] + dxr[0].astype(F32)
    for i in range(1, 8):
        chip_copy(i).wait()
        total = total + dfr[i].astype(F32)
    dx_out[...] = total

    for copy in started:
        copy.wait_send()
    for j in range(chunks):
        for way in range(2):
            a1(j, way).wait_send()
            a2(j, way).wait_send()
    for j in range(chunks - 2, chunks):
        for m in range(3):
            out_copy(j, m).wait()


def per_device(codes, scales, mask, cot, wg, wu, wo):
    tb, dl = codes.shape
    fl = wg.shape[1]
    chunks = fl // W
    dims = (tb, dl, chunks)
    tile = 2 * tb + FOOT
    vmem = pl.BlockSpec(memory_space=pltpu.VMEM)
    hbm = pl.BlockSpec(memory_space=pl.ANY)
    dma = pltpu.SemaphoreType.DMA
    weight = jax.ShapeDtypeStruct((dl, fl), F32)
    return pl.pallas_call(
        functools.partial(kernel, dims),
        out_shape=(jax.ShapeDtypeStruct((tb, dl), F32), weight, weight, weight),
        in_specs=[vmem] * 4 + [hbm] * 3,
        out_specs=(vmem, hbm, hbm, hbm),
        scratch_shapes=[
            pltpu.VMEM((16 * tb, 2 * dl), BF16),
            pltpu.VMEM((chunks, dl, 3 * W), BF16),
            pltpu.VMEM((3, 4, 2, tile, 3 * W), jnp.int16),
            pltpu.VMEM((chunks, 2, tile, 3 * W), jnp.int16),
            pltpu.VMEM((chunks, 2, 2, tile, 3 * W), jnp.int16),
            pltpu.VMEM((chunks, 16 * tb, 3 * W), BF16),
            pltpu.VMEM((16 * tb, dl), F32),
            pltpu.VMEM((chunks, dl, 3 * W), BF16),
            pltpu.VMEM((chunks, dl, 3 * W), BF16),
            pltpu.VMEM((2, 3, dl, W), F32),
            pltpu.VMEM((8, tb, dl), BF16),
            pltpu.VMEM((8, tb, dl), BF16),
            pltpu.VMEM((8, tb, dl), BF16),
            dma((chunks, 3)),
            dma((17,)), dma((17,)),
            dma((chunks, 2)), dma((chunks, 2)),
            dma((chunks, 2)), dma((chunks, 2)),
            dma((chunks, 2)), dma((chunks, 2)),
            dma((chunks, 2)), dma((chunks, 2)),
            dma((chunks,)), dma((chunks,)),
            dma((chunks, 3)),
            dma((1,)), dma((1,)),
            dma((8,)), dma((8,)),
        ],
        compiler_params=pltpu.CompilerParams(
            collective_id=0, has_side_effects=True, vmem_limit_bytes=67043328
        ),
        name="ffn_backward",
    )(codes, scales, mask[:, None], cot, wg, wu, wo)


def solution(mesh):
    tokens = P(("dp", "col"), "row")
    weights = P("row", "col")
    return jax.shard_map(
        per_device,
        mesh=mesh,
        in_specs=(tokens, tokens, P(("dp", "col")), tokens, weights, weights, weights),
        out_specs=(tokens, weights, weights, weights),
        check_vma=False,
    )
```

```python
import functools

import jax
import jax.numpy as jnp
from jax import lax
from jax.experimental import pallas as pl
from jax.experimental.pallas import tpu as pltpu
from jax.sharding import PartitionSpec as P

MESH = pl.DeviceIdType.MESH
ROOT = 0.7978845608028654
CUBIC = 0.044715
W = 128
KEEP = 6
FOOT = 8
F32 = jnp.float32
BF16 = jnp.bfloat16


def gelu_pair(values):
    inside = ROOT * (values + CUBIC * values * values * values)
    tangent = jnp.tanh(inside)
    activated = 0.5 * values * (1.0 + tangent)
    derivative = 0.5 * (1.0 + tangent) + 0.5 * values * (1.0 - tangent * tangent) * ROOT * (
        1.0 + 3.0 * CUBIC * values * values
    )
    return activated, derivative


def coded(part):
    most = jnp.maximum(jnp.max(jnp.abs(part), axis=0, keepdims=True), 1e-30)
    power = jnp.floor(jnp.log(most) * 1.4426950408889634) + 1.0
    units = jnp.round(part * jnp.exp2(15.0 - power))
    units = jnp.clip(units, -32767.0, 32767.0).astype(jnp.int32).astype(jnp.int16)
    foot = jnp.broadcast_to(power, (FOOT, part.shape[1])).astype(jnp.int32).astype(jnp.int16)
    return units, foot


def store_coded(tile, lanes, part):
    rows = part.shape[0]
    units, foot = coded(part)
    tile[pl.ds(0, rows), lanes] = units
    tile[pl.ds(rows, FOOT), lanes] = foot


def decoded(tile, rows, lanes):
    power = tile[pl.ds(rows, FOOT), lanes].astype(jnp.int32).astype(F32)[0:1]
    units = tile[pl.ds(0, rows), lanes].astype(jnp.int32).astype(F32)
    return units * jnp.exp2(power - 15.0)


def kernel(
    dims,
    codes, scales, mask, cot, wg, wu, wo,
    dx_out, own_out, got_out,
    sl, wc, pb, r1, r2, guh, dx, dws, dwr, relay, dxs, dxr, ybuf, y2, zbuf,
    w_sem, ag_s, ag_r, rs1_s, rs1_r, rs2_s, rs2_r, a1_s, a1_r, a2_s, a2_r,
    p1_s, p1_r, p2_s, p2_r, own_sem, got_sem, dxc_s, dxc_r, y1_s, y1_r, y2_s, y2_r, z_s, z_r,
):
    tb, dl, chunks = dims
    blk = 4 * tb
    units = 4 * chunks
    x = lax.axis_index("row")
    col = lax.axis_index("col")
    dp = lax.axis_index("dp")
    core = lax.rem(col, 2)
    y = lax.rem(col // 2, 4)
    z = col // 8
    opp = lax.rem(x + 2, 4)

    def at_col(dz, dy, dc):
        zz = (1 - z) if dz else z
        cc = (1 - core) if dc else core
        return {"col": (zz * 4 + lax.rem(y + dy, 4)) * 2 + cc}

    def beside(way):
        return lax.rem(x + 1 + 2 * way, 4)

    def to_row(way):
        return {"row": beside(way)}

    partner = at_col(0, 0, 1)
    up, down = at_col(0, 1, 0), at_col(0, 3, 0)
    near = at_col(1, 0, 0)
    far = dict(near, dp=1 - dp)

    barrier = pltpu.get_barrier_semaphore()
    peers = [to_row(0), to_row(1), partner, up, down, near, far]
    for peer in peers:
        pl.semaphore_signal(barrier, inc=1, device_id=peer, device_id_type=MESH)

    def weight_copy(j, m, src):
        return pltpu.make_async_copy(
            src.at[:, pl.ds(j * W, W)], wc.at[j, :, pl.ds(m * W, W)], w_sem.at[j, m]
        )

    for j in range(chunks):
        for m, src in enumerate((wg, wu, wo)):
            weight_copy(j, m, src).start()

    nb = scales.shape[0]
    flat = jnp.concatenate(
        [scales[...].astype(F32), jnp.broadcast_to(mask[...], (8, tb)).astype(F32),
         jnp.zeros((128 - nb - 8, tb), F32)], axis=0,
    )
    tall = jnp.transpose(flat)
    for k in range(nb):
        lanes = pl.ds(k * 128, 128)
        level = (2 * codes[:, lanes] - 3).astype(F32) * tall[:, k : k + 1]
        sl[pl.ds(0, tb), lanes] = (level * 0.0625).astype(BF16)
        live = cot[:, lanes].astype(F32) * tall[:, nb : nb + 1]
        sl[pl.ds(0, tb), pl.ds(dl + k * 128, 128)] = live.astype(BF16)

    with jax.named_scope("barrier"):
        pl.semaphore_wait(barrier, len(peers))

    def remote(src, dst, s_sem, r_sem, device):
        return pltpu.make_async_remote_copy(
            src_ref=src, dst_ref=dst, send_sem=s_sem, recv_sem=r_sem,
            device_id=device, device_id_type=MESH,
        )

    def slot(b, zr, cr):
        return (b * 4 + zr * 2 + cr) * tb

    def rows(start, count):
        return sl.at[pl.ds(start, count)]

    started = []

    def gather(kind, src, dst, count, device):
        copy = remote(rows(src, count), rows(dst, count), ag_s.at[kind], ag_r.at[kind], device)
        copy.start()
        started.append(copy)

    def arrived(kind, dst, count):
        remote(rows(dst, count), rows(dst, count), ag_s.at[kind], ag_r.at[kind], partner).wait_recv()

    def to_core(kind, b, zr):
        gather(9 + kind, slot(b, zr, 0), slot(b, zr, 1), tb, partner)

    part = tb // 2
    gather(0, slot(0, 0, 0), slot(0, 1, 0), tb, near)
    gather(1, slot(0, 0, 0), slot(1, 0, 0), tb, up)
    gather(2, slot(0, 0, 0), slot(2, 0, 0), tb, down)
    to_core(0, 0, 0)
    for j in range(chunks):
        for m, src in enumerate((wg, wu, wo)):
            weight_copy(j, m, src).wait()

    def unit(u):
        s = (u // 8 + 1) // 2
        return (1 - s) * lax.rem(u, 2) + s * (u // 4), (1 - s) * (u // 2) + s * lax.rem(u, 4)

    def unit_of(j, b):
        s = (j // 2 + 1) // 2
        return (1 - s) * (2 * b + j) + s * (4 * j + b)

    def held(u):
        return pb.at[lax.rem(u, KEEP)]

    def grad_rows(j, b, owner):
        return guh.at[j, pl.ds(pl.multiple_of((b * 4 + owner) * tb, tb), tb)]

    def rs1(u, way):
        return remote(held(u).at[opp], r1.at[u], rs1_s.at[u], rs1_r.at[u], to_row(way))

    def rs2(u, way):
        return remote(
            held(u).at[beside(way)], r2.at[u, way], rs2_s.at[u, way], rs2_r.at[u, way], to_row(way)
        )

    def a1(u, way, owner):
        j, b = unit(u)
        ref = grad_rows(j, b, owner)
        return remote(ref, ref, a1_s.at[u, way], a1_r.at[u, way], to_row(way))

    def a2(u, owner):
        j, b = unit(u)
        ref = grad_rows(j, b, owner)
        return remote(ref, ref, a2_s.at[u], a2_r.at[u], to_row(lax.rem(b, 2)))

    def sent(u):
        rs1(u, lax.rem(unit(u)[1], 2)).wait_send()
        for way in range(2):
            rs2(u, way).wait_send()

    def stage_f(u):
        j, b = unit(u)
        if isinstance(u, int):
            if u >= KEEP:
                sent(u - KEEP)
        else:
            sent(u - KEEP)
        where = pl.ds(pl.multiple_of(b * blk, blk), blk)
        both = jnp.dot(
            sl[where, pl.ds(0, dl)], wc[j, :, pl.ds(0, 2 * W)], preferred_element_type=F32
        )
        back = jnp.dot(
            sl[where, pl.ds(dl, dl)], wc[j, :, pl.ds(2 * W, W)], preferred_element_type=F32
        )
        for o in range(4):
            tile = held(u).at[o]
            store_coded(tile, pl.ds(0, 2 * W), both[o * tb : (o + 1) * tb])
            store_coded(tile, pl.ds(2 * W, W), back[o * tb : (o + 1) * tb])
        rs1(u, lax.rem(b, 2)).start()

    def stage_r(u):
        j, b = unit(u)
        way = lax.rem(b, 2)
        rs2(u, 1 - way).start()
        with jax.named_scope("r_wait"):
            rs1(u, way).wait_recv()
        tile = held(u).at[beside(way)]
        for m in range(3):
            lanes = pl.ds(m * W, W)
            total = decoded(tile, tb, lanes) + decoded(r1.at[u], tb, lanes)
            store_coded(tile, lanes, total)
        rs2(u, way).start()

    def stage_a(u):
        j, b = unit(u)
        with jax.named_scope("a_wait"):
            for way in range(2):
                rs2(u, way).wait_recv()
        tiles = (held(u).at[x], r2.at[u, 0], r2.at[u, 1])
        powers = [
            [
                jnp.exp2(t[pl.ds(tb, FOOT), pl.ds(m * W, W)].astype(jnp.int32).astype(F32)[0:1] - 15.0)
                for t in tiles
            ]
            for m in range(3)
        ]
        step = tb // 2

        def body(k, carry):
            some = pl.ds(pl.multiple_of(k * step, step), step)
            sums = []
            for m in range(3):
                total = None
                for t, power in zip(tiles, powers[m]):
                    term = t[some, pl.ds(m * W, W)].astype(jnp.int32).astype(F32) * power
                    total = term if total is None else total + term
                sums.append(total)
            gate, up_part, back = sums
            activated, derivative = gelu_pair(gate)
            to = pl.ds(pl.multiple_of((b * 4 + x) * tb + k * step, step), step)
            guh[j, to, pl.ds(0, W)] = (back * up_part * derivative).astype(BF16)
            guh[j, to, pl.ds(W, W)] = (back * activated).astype(BF16)
            guh[j, to, pl.ds(2 * W, W)] = (activated * up_part).astype(BF16)
            return carry

        lax.fori_loop(0, 2, body, 0)
        for way in range(2):
            a1(u, way, x).start()

    def stage_w(u):
        b = unit(u)[1]
        way = lax.rem(b, 2)
        with jax.named_scope("w_wait"):
            a1(u, way, beside(1 - way)).wait_recv()
        a2(u, beside(1 - way)).start()

    def stage_dx(j):
        with jax.named_scope("b_wait"):
            for b in range(4):
                u = unit_of(j, b)
                a1(u, 1 - b % 2, beside(b % 2)).wait_recv()
                a2(u, opp).wait_recv()

        def body(k, carry):
            where = pl.ds(pl.multiple_of(k * 2 * tb, 2 * tb), 2 * tb)
            more = lax.dot_general(
                guh[j, where, pl.ds(0, 2 * W)], wc[j, :, pl.ds(0, 2 * W)],
                (((1,), (1,)), ((), ())), preferred_element_type=F32,
            )
            dx[where, :] = dx[where, :] + more
            return carry

        lax.fori_loop(0, 8, body, 0)

    half = dl // 2

    def p1(j, way):
        part_of = dws.at[j, pl.ds(way * half, half)]
        return remote(
            part_of, relay.at[j, way], p1_s.at[j, way], p1_r.at[j, way], (near, far)[way]
        )

    def p2(j, way):
        return remote(
            relay.at[j, way], dwr.at[j, pl.ds(way * half, half)], p2_s.at[j, way],
            p2_r.at[j, way], (far, near)[way],
        )

    def own_copy(j):
        return pltpu.make_async_copy(dws.at[j], own_out.at[j], own_sem.at[j])

    def got_copy(j):
        return pltpu.make_async_copy(dwr.at[j], got_out.at[j], got_sem.at[j])

    def stage_dw(j):
        def body(k, carry):
            where = pl.ds(pl.multiple_of(k * 256, 256), 256)
            some = lax.dot_general(
                sl[:, where], guh[j, :, pl.ds(0, 2 * W)],
                (((0,), (0,)), ((), ())), preferred_element_type=F32,
            )
            dws[j, where, pl.ds(0, 2 * W)] = some.astype(BF16)
            last = lax.dot_general(
                sl[:, pl.ds(pl.multiple_of(dl + k * 256, 256), 256)], guh[j, :, pl.ds(2 * W, W)],
                (((0,), (0,)), ((), ())), preferred_element_type=F32,
            )
            dws[j, where, pl.ds(2 * W, W)] = last.astype(BF16)
            return carry

        lax.fori_loop(0, dl // 256, body, 0)
        for way in range(2):
            p1(j, way).start()
        own_copy(j).start()

    def stage_g(j):
        for way in range(2):
            with jax.named_scope("g_wait"):
                p1(j, way).wait_recv()
            p2(j, way).start()

    def stage_e(j):
        with jax.named_scope("e_wait"):
            for way in range(2):
                p2(j, way).wait_recv()
        got_copy(j).start()

    arrived(0, slot(0, 1, 0), tb)
    gather(3, slot(0, 1, 0), slot(1, 1, 0), tb, up)
    gather(4, slot(0, 1, 0), slot(2, 1, 0), tb, down)
    to_core(1, 0, 1)
    arrived(1, slot(1, 0, 0), tb)
    gather(5, slot(1, 0, 0), slot(3, 0, 0), part, up)
    to_core(2, 1, 0)
    arrived(2, slot(2, 0, 0), tb)
    gather(6, slot(2, 0, 0) + part, slot(3, 0, 0) + part, part, down)
    to_core(3, 2, 0)
    arrived(9, slot(0, 0, 1), tb)
    arrived(10, slot(0, 1, 1), tb)

    def run(stage, *which):
        for u in which:
            with jax.named_scope(f"{stage.__name__}_{u}"):
                stage(u)

    run(stage_f, 0, 1)
    run(stage_r, 0, 1)
    run(stage_a, 0, 1)
    with jax.named_scope("ag1"):
        arrived(3, slot(1, 1, 0), tb)
        gather(7, slot(1, 1, 0), slot(3, 1, 0), part, up)
        to_core(4, 1, 1)
        arrived(4, slot(2, 1, 0), tb)
        gather(8, slot(2, 1, 0) + part, slot(3, 1, 0) + part, part, down)
        to_core(5, 2, 1)
    run(stage_w, 0, 1)
    with jax.named_scope("ag2"):
        arrived(11, slot(1, 0, 1), tb)
        arrived(13, slot(1, 1, 1), tb)
        arrived(12, slot(2, 0, 1), tb)
        arrived(14, slot(2, 1, 1), tb)
    run(stage_f, 2, 3, 4, 5)
    run(stage_r, 2, 3)
    run(stage_a, 2, 3)
    run(stage_r, 4, 5)
    with jax.named_scope("ag3"):
        arrived(5, slot(3, 0, 0), part)
        arrived(6, slot(3, 0, 0) + part, part)
        to_core(6, 3, 0)
        arrived(7, slot(3, 1, 0), part)
        arrived(8, slot(3, 1, 0) + part, part)
        to_core(7, 3, 1)
        arrived(15, slot(3, 0, 1), tb)
        arrived(16, slot(3, 1, 1), tb)
    run(stage_f, 6, 7)
    dx[...] = jnp.zeros_like(dx)

    last = chunks - 1

    def step(t, carry):
        def at(lag, fn, least=0, most=units):
            @pl.when(jnp.logical_and(t - lag >= least, t - lag < most))
            def _():
                with jax.named_scope(fn.__name__):
                    fn(t - lag)

        def at_end(lag, *fns):
            j, b = unit(t - lag)

            @pl.when(jnp.logical_and(jnp.logical_and(t - lag >= 0, b == 3), j < last))
            def _():
                for fn in fns:
                    with jax.named_scope(fn.__name__):
                        fn(j)

        at(0, stage_f)
        at(2, stage_r)
        at(4, stage_a)
        at(6, stage_w)
        at_end(8, stage_dx, stage_dw)
        at_end(11, stage_g)
        at_end(14, stage_e)
        return carry

    lax.fori_loop(8, units + 7, step, 0)

    with jax.named_scope("dx_last"):
        stage_dx(last)

    def dx_rows(b, zr, cr):
        return pl.ds(slot(b, zr, cr), tb)

    def core_copy(b):
        return remote(dxs.at[b], dxr.at[b], dxc_s.at[b], dxc_r.at[b], partner)

    for b in (3, 1, 2, 0):
        for zr in range(2):
            dxs[b, zr] = dx[dx_rows(b, zr, 1), :].astype(BF16)
        core_copy(b).start()
    with jax.named_scope("dw_last"):
        stage_dw(last)

    def y1_copy(zr):
        return remote(dxs.at[3, zr], ybuf.at[zr], y1_s.at[zr], y1_r.at[zr], (up, down)[zr])

    def y2_copy(way, zr):
        return remote(
            dxs.at[2 - way, zr], y2.at[way, zr], y2_s.at[way, zr], y2_r.at[way, zr],
            (up, down)[way],
        )

    core_copy(3).wait()
    for zr in range(2):
        dxs[3, zr] = (dx[dx_rows(3, zr, 0), :] + dxr[3, zr].astype(F32)).astype(BF16)
        y1_copy(zr).start()
    for way in range(2):
        b, zr = 2 - way, 1 - way
        core_copy(b).wait()
        dxs[b, zr] = (dx[dx_rows(b, zr, 0), :] + dxr[b, zr].astype(F32)).astype(BF16)
        y2_copy(way, zr).start()
    with jax.named_scope("y1_wait"):
        for way in range(2):
            y1_copy(way).wait_recv()
            b, zr = 2 - way, way
            total = dx[dx_rows(b, zr, 0), :] + dxr[b, zr].astype(F32) + ybuf[zr].astype(F32)
            dxs[b, zr] = total.astype(BF16)
            y2_copy(way, zr).start()
    core_copy(0).wait()
    for zr in range(2):
        dx[dx_rows(0, zr, 0), :] = dx[dx_rows(0, zr, 0), :] + dxr[0, zr].astype(F32)
    with jax.named_scope("g_last"):
        stage_g(last)
    with jax.named_scope("e_prev"):
        stage_e(last - 1)
    z_copy = remote(dxs.at[0, 1], zbuf, z_s.at[0], z_r.at[0], near)
    with jax.named_scope("y2_wait"):
        for way in range(2):
            y2_copy(way, 1).wait_recv()
        total = dx[dx_rows(0, 1, 0), :] + y2[0, 1].astype(F32) + y2[1, 1].astype(F32)
        dxs[0, 1] = total.astype(BF16)
        z_copy.start()
        for way in range(2):
            y2_copy(way, 0).wait_recv()
        total = dx[dx_rows(0, 0, 0), :] + y2[0, 0].astype(F32) + y2[1, 0].astype(F32)
    with jax.named_scope("z_wait"):
        z_copy.wait()
    dx_out[...] = total + zbuf[...].astype(F32)
    with jax.named_scope("e_last"):
        stage_e(last)

    with jax.named_scope("end"):
        for copy in started:
            copy.wait_send()
        for u in range(units - KEEP, units):
            sent(u)
        for u in range(units):
            for way in range(2):
                a1(u, way, x).wait_send()
            a2(u, opp).wait_send()
        for j in range(chunks):
            for way in range(2):
                p1(j, way).wait_send()
                p2(j, way).wait_send()
            own_copy(j).wait()
            got_copy(j).wait()
        for zr in range(2):
            y1_copy(zr).wait_send()
            for way in range(2):
                y2_copy(way, zr).wait_send()


def combine(own, got, dx, dx_out, g_out, u_out, o_out):
    for j in range(own.shape[0]):
        for m, out in enumerate((g_out, u_out, o_out)):
            lanes = pl.ds(m * W, W)
            out[:, pl.ds(j * W, W)] = own[j, :, lanes].astype(F32) + got[j, :, lanes].astype(F32)
    dx_out[...] = dx[...]


def per_device(codes, scales, mask, cot, wg, wu, wo):
    tb, dl = codes.shape
    fl = wg.shape[1]
    chunks = fl // W
    units = 4 * chunks
    dims = (tb, dl, chunks)
    tile = tb + FOOT
    vmem = pl.BlockSpec(memory_space=pltpu.VMEM)
    hbm = pl.BlockSpec(memory_space=pl.ANY)
    dma = pltpu.SemaphoreType.DMA
    grads = jax.ShapeDtypeStruct((chunks, dl, 3 * W), BF16)
    dx, own, got = pl.pallas_call(
        functools.partial(kernel, dims),
        out_shape=(jax.ShapeDtypeStruct((tb, dl), F32), grads, grads),
        in_specs=[vmem] * 4 + [hbm] * 3,
        out_specs=(vmem, hbm, hbm),
        scratch_shapes=[
            pltpu.VMEM((16 * tb, 2 * dl), BF16),
            pltpu.VMEM((chunks, dl, 3 * W), BF16),
            pltpu.VMEM((KEEP, 4, tile, 3 * W), jnp.int16),
            pltpu.VMEM((units, tile, 3 * W), jnp.int16),
            pltpu.VMEM((units, 2, tile, 3 * W), jnp.int16),
            pltpu.VMEM((chunks, 16 * tb, 3 * W), BF16),
            pltpu.VMEM((16 * tb, dl), F32),
            pltpu.VMEM((chunks, dl, 3 * W), BF16),
            pltpu.VMEM((chunks, dl, 3 * W), BF16),
            pltpu.VMEM((chunks, 2, dl // 2, 3 * W), BF16),
            pltpu.VMEM((4, 2, tb, dl), BF16),
            pltpu.VMEM((4, 2, tb, dl), BF16),
            pltpu.VMEM((2, tb, dl), BF16),
            pltpu.VMEM((2, 2, tb, dl), BF16),
            pltpu.VMEM((tb, dl), BF16),
            dma((chunks, 3)),
            dma((17,)), dma((17,)),
            dma((units,)), dma((units,)),
            dma((units, 2)), dma((units, 2)),
            dma((units, 2)), dma((units, 2)),
            dma((units,)), dma((units,)),
            dma((chunks, 2)), dma((chunks, 2)),
            dma((chunks, 2)), dma((chunks, 2)),
            dma((chunks,)), dma((chunks,)),
            dma((4,)), dma((4,)),
            dma((2,)), dma((2,)),
            dma((2, 2)), dma((2, 2)),
            dma((1,)), dma((1,)),
        ],
        compiler_params=pltpu.CompilerParams(
            collective_id=0, has_side_effects=True, vmem_limit_bytes=67043328
        ),
        name="ffn_backward",
    )(codes, scales.T, mask[None, :], cot, wg, wu, wo)
    weight = jax.ShapeDtypeStruct((dl, fl), F32)
    steps = 8
    rows = dl // steps
    return pl.pallas_call(
        combine,
        grid=(steps,),
        out_shape=(jax.ShapeDtypeStruct((tb, dl), F32), weight, weight, weight),
        in_specs=[
            pl.BlockSpec((chunks, rows, 3 * W), lambda i: (0, i, 0)),
            pl.BlockSpec((chunks, rows, 3 * W), lambda i: (0, i, 0)),
            pl.BlockSpec((tb // steps, dl), lambda i: (i, 0)),
        ],
        out_specs=[pl.BlockSpec((tb // steps, dl), lambda i: (i, 0))]
        + [pl.BlockSpec((rows, fl), lambda i: (i, 0))] * 3,
        name="combine",
    )(own, got, dx)


def solution(mesh):
    tokens = P(("dp", "col"), "row")
    weights = P("row", "col")
    return jax.shard_map(
        per_device,
        mesh=mesh,
        in_specs=(tokens, tokens, P(("dp", "col")), tokens, weights, weights, weights),
        out_specs=(tokens, weights, weights, weights),
        check_vma=False,
    )
```

```python
import functools

import jax
import jax.numpy as jnp
from jax import lax
from jax.experimental import pallas as pl
from jax.experimental.pallas import tpu as pltpu
from jax.sharding import PartitionSpec as P

MESH = pl.DeviceIdType.MESH
ROOT = 0.7978845608028654
CUBIC = 0.044715
W = 128
KEEP = 6
FOOT = 8
F32 = jnp.float32
BF16 = jnp.bfloat16


def gelu_pair(values):
    inside = ROOT * (values + CUBIC * values * values * values)
    tangent = jnp.tanh(inside)
    activated = 0.5 * values * (1.0 + tangent)
    derivative = 0.5 * (1.0 + tangent) + 0.5 * values * (1.0 - tangent * tangent) * ROOT * (
        1.0 + 3.0 * CUBIC * values * values
    )
    return activated, derivative


def coded(part):
    most = jnp.maximum(jnp.max(jnp.abs(part), axis=0, keepdims=True), 1e-30)
    power = jnp.floor(jnp.log(most) * 1.4426950408889634) + 1.0
    units = jnp.round(part * jnp.exp2(15.0 - power))
    units = jnp.clip(units, -32767.0, 32767.0).astype(jnp.int32).astype(jnp.int16)
    foot = jnp.broadcast_to(power, (FOOT, part.shape[1])).astype(jnp.int32).astype(jnp.int16)
    return units, foot


def store_coded(tile, lanes, part):
    rows = part.shape[0]
    units, foot = coded(part)
    tile[pl.ds(0, rows), lanes] = units
    tile[pl.ds(rows, FOOT), lanes] = foot


def decoded(tile, rows, lanes):
    power = tile[pl.ds(rows, FOOT), lanes].astype(jnp.int32).astype(F32)[0:1]
    units = tile[pl.ds(0, rows), lanes].astype(jnp.int32).astype(F32)
    return units * jnp.exp2(power - 15.0)


def kernel(
    dims,
    codes, scales, mask, cot, wg, wu, wo,
    dx_out, own_out, got_out,
    sl, wc, pb, r1, r2, guh, dx, dws, dwr, relay, dxs, dxr, ybuf, y2, zbuf,
    w_sem, ag_s, ag_r, rs1_s, rs1_r, rs2_s, rs2_r, a1_s, a1_r, a2_s, a2_r,
    p1_s, p1_r, p2_s, p2_r, own_sem, got_sem, dxc_s, dxc_r, y1_s, y1_r, y2_s, y2_r, z_s, z_r,
):
    tb, dl, chunks = dims
    blk = 4 * tb
    units = 4 * chunks
    x = lax.axis_index("row")
    col = lax.axis_index("col")
    dp = lax.axis_index("dp")
    core = lax.rem(col, 2)
    y = lax.rem(col // 2, 4)
    z = col // 8
    opp = lax.rem(x + 2, 4)

    def at_col(dz, dy, dc):
        zz = (1 - z) if dz else z
        cc = (1 - core) if dc else core
        return {"col": (zz * 4 + lax.rem(y + dy, 4)) * 2 + cc}

    def beside(way):
        return lax.rem(x + 1 + 2 * way, 4)

    def to_row(way):
        return {"row": beside(way)}

    partner = at_col(0, 0, 1)
    up, down = at_col(0, 1, 0), at_col(0, 3, 0)
    near = at_col(1, 0, 0)
    far = dict(near, dp=1 - dp)

    barrier = pltpu.get_barrier_semaphore()
    peers = [to_row(0), to_row(1), partner, up, down, near, far]
    for peer in peers:
        pl.semaphore_signal(barrier, inc=1, device_id=peer, device_id_type=MESH)

    def weight_copy(j, m, src):
        return pltpu.make_async_copy(
            src.at[:, pl.ds(j * W, W)], wc.at[j, :, pl.ds(m * W, W)], w_sem.at[j, m]
        )

    for j in range(chunks):
        for m, src in enumerate((wg, wu, wo)):
            weight_copy(j, m, src).start()

    nb = scales.shape[0]
    flat = jnp.concatenate(
        [scales[...].astype(F32), jnp.broadcast_to(mask[...], (8, tb)).astype(F32),
         jnp.zeros((128 - nb - 8, tb), F32)], axis=0,
    )
    tall = jnp.transpose(flat)
    for k in range(nb):
        lanes = pl.ds(k * 128, 128)
        level = (2 * codes[:, lanes] - 3).astype(F32) * tall[:, k : k + 1]
        sl[pl.ds(0, tb), lanes] = (level * 0.0625).astype(BF16)
        live = cot[:, lanes].astype(F32) * tall[:, nb : nb + 1]
        sl[pl.ds(0, tb), pl.ds(dl + k * 128, 128)] = live.astype(BF16)

    with jax.named_scope("barrier"):
        pl.semaphore_wait(barrier, len(peers))

    def remote(src, dst, s_sem, r_sem, device):
        return pltpu.make_async_remote_copy(
            src_ref=src, dst_ref=dst, send_sem=s_sem, recv_sem=r_sem,
            device_id=device, device_id_type=MESH,
        )

    def slot(b, zr, cr):
        return (b * 4 + zr * 2 + cr) * tb

    def rows(start, count):
        return sl.at[pl.ds(start, count)]

    started = []

    def gather(kind, src, dst, count, device):
        copy = remote(rows(src, count), rows(dst, count), ag_s.at[kind], ag_r.at[kind], device)
        copy.start()
        started.append(copy)

    def arrived(kind, dst, count):
        remote(rows(dst, count), rows(dst, count), ag_s.at[kind], ag_r.at[kind], partner).wait_recv()

    def to_core(kind, b, zr):
        gather(9 + kind, slot(b, zr, 0), slot(b, zr, 1), tb, partner)

    part = tb // 2
    gather(0, slot(0, 0, 0), slot(0, 1, 0), tb, near)
    gather(1, slot(0, 0, 0), slot(1, 0, 0), tb, up)
    gather(2, slot(0, 0, 0), slot(2, 0, 0), tb, down)
    to_core(0, 0, 0)
    for j in range(chunks):
        for m, src in enumerate((wg, wu, wo)):
            weight_copy(j, m, src).wait()

    def place(u):
        s = (u // 8 + 1) // 2
        return s, (1 - s) * (u // 2) + s * lax.rem(u, 4)

    def unit(u):
        s, k = place(u)
        return (1 - s) * lax.rem(u, 2) + s * (u // 4), (1 - s) * k + s * (3 - k)

    def held(u):
        return pb.at[lax.rem(u, KEEP)]

    def grad_rows(j, b, owner):
        return guh.at[j, pl.ds(pl.multiple_of((b * 4 + owner) * tb, tb), tb)]

    def rs1(u, way):
        return remote(held(u).at[opp], r1.at[u], rs1_s.at[u], rs1_r.at[u], to_row(way))

    def rs2(u, way):
        return remote(
            held(u).at[beside(way)], r2.at[u, way], rs2_s.at[u, way], rs2_r.at[u, way], to_row(way)
        )

    def a1(u, way, owner):
        j, b = unit(u)
        ref = grad_rows(j, b, owner)
        return remote(ref, ref, a1_s.at[u, way], a1_r.at[u, way], to_row(way))

    def a2(u, owner):
        j, b = unit(u)
        ref = grad_rows(j, b, owner)
        return remote(ref, ref, a2_s.at[u], a2_r.at[u], to_row(lax.rem(b, 2)))

    def sent(u):
        rs1(u, lax.rem(unit(u)[1], 2)).wait_send()
        for way in range(2):
            rs2(u, way).wait_send()

    def stage_f(u):
        j, b = unit(u)
        if isinstance(u, int):
            if u >= KEEP:
                sent(u - KEEP)
        else:
            sent(u - KEEP)
        where = pl.ds(pl.multiple_of(b * blk, blk), blk)
        both = jnp.dot(
            sl[where, pl.ds(0, dl)], wc[j, :, pl.ds(0, 2 * W)], preferred_element_type=F32
        )
        back = jnp.dot(
            sl[where, pl.ds(dl, dl)], wc[j, :, pl.ds(2 * W, W)], preferred_element_type=F32
        )
        for o in range(4):
            tile = held(u).at[o]
            store_coded(tile, pl.ds(0, 2 * W), both[o * tb : (o + 1) * tb])
            store_coded(tile, pl.ds(2 * W, W), back[o * tb : (o + 1) * tb])
        rs1(u, lax.rem(b, 2)).start()

    def stage_r(u):
        j, b = unit(u)
        way = lax.rem(b, 2)
        rs2(u, 1 - way).start()
        with jax.named_scope("r_wait"):
            rs1(u, way).wait_recv()
        tile = held(u).at[beside(way)]
        for m in range(3):
            lanes = pl.ds(m * W, W)
            total = decoded(tile, tb, lanes) + decoded(r1.at[u], tb, lanes)
            store_coded(tile, lanes, total)
        rs2(u, way).start()

    def stage_a(u):
        j, b = unit(u)
        with jax.named_scope("a_wait"):
            for way in range(2):
                rs2(u, way).wait_recv()
        tiles = (held(u).at[x], r2.at[u, 0], r2.at[u, 1])
        powers = [
            [
                jnp.exp2(t[pl.ds(tb, FOOT), pl.ds(m * W, W)].astype(jnp.int32).astype(F32)[0:1] - 15.0)
                for t in tiles
            ]
            for m in range(3)
        ]
        step = tb // 2

        def body(k, carry):
            some = pl.ds(pl.multiple_of(k * step, step), step)
            sums = []
            for m in range(3):
                total = None
                for t, power in zip(tiles, powers[m]):
                    term = t[some, pl.ds(m * W, W)].astype(jnp.int32).astype(F32) * power
                    total = term if total is None else total + term
                sums.append(total)
            gate, up_part, back = sums
            activated, derivative = gelu_pair(gate)
            to = pl.ds(pl.multiple_of((b * 4 + x) * tb + k * step, step), step)
            guh[j, to, pl.ds(0, W)] = (back * up_part * derivative).astype(BF16)
            guh[j, to, pl.ds(W, W)] = (back * activated).astype(BF16)
            guh[j, to, pl.ds(2 * W, W)] = (activated * up_part).astype(BF16)
            return carry

        lax.fori_loop(0, 2, body, 0)
        for way in range(2):
            a1(u, way, x).start()

    def stage_w(u):
        b = unit(u)[1]
        way = lax.rem(b, 2)
        with jax.named_scope("w_wait"):
            a1(u, way, beside(1 - way)).wait_recv()
        a2(u, beside(1 - way)).start()

    def stage_dx(u):
        j, b = unit(u)
        way = lax.rem(b, 2)
        with jax.named_scope("b_wait"):
            a1(u, 1 - way, beside(way)).wait_recv()
            a2(u, opp).wait_recv()
        where = pl.ds(pl.multiple_of(b * blk, blk), blk)
        more = lax.dot_general(
            guh[j, where, pl.ds(0, 2 * W)], wc[j, :, pl.ds(0, 2 * W)],
            (((1,), (1,)), ((), ())), preferred_element_type=F32,
        )
        dx[where, :] = dx[where, :] + more

    half = dl // 2

    def p1(j, way):
        part_of = dws.at[j, pl.ds(way * half, half)]
        return remote(
            part_of, relay.at[j, way], p1_s.at[j, way], p1_r.at[j, way], (near, far)[way]
        )

    def p2(j, way):
        return remote(
            relay.at[j, way], dwr.at[j, pl.ds(way * half, half)], p2_s.at[j, way],
            p2_r.at[j, way], (far, near)[way],
        )

    def own_copy(j):
        return pltpu.make_async_copy(dws.at[j], own_out.at[j], own_sem.at[j])

    def got_copy(j):
        return pltpu.make_async_copy(dwr.at[j], got_out.at[j], got_sem.at[j])

    def stage_dw(j):
        def body(k, carry):
            where = pl.ds(pl.multiple_of(k * 256, 256), 256)
            some = lax.dot_general(
                sl[:, where], guh[j, :, pl.ds(0, 2 * W)],
                (((0,), (0,)), ((), ())), preferred_element_type=F32,
            )
            dws[j, where, pl.ds(0, 2 * W)] = some.astype(BF16)
            last = lax.dot_general(
                sl[:, pl.ds(pl.multiple_of(dl + k * 256, 256), 256)], guh[j, :, pl.ds(2 * W, W)],
                (((0,), (0,)), ((), ())), preferred_element_type=F32,
            )
            dws[j, where, pl.ds(2 * W, W)] = last.astype(BF16)
            return carry

        lax.fori_loop(0, dl // 256, body, 0)
        for way in range(2):
            p1(j, way).start()
        own_copy(j).start()

    def stage_g(j):
        for way in range(2):
            with jax.named_scope("g_wait"):
                p1(j, way).wait_recv()
            p2(j, way).start()

    def stage_e(j):
        with jax.named_scope("e_wait"):
            for way in range(2):
                p2(j, way).wait_recv()
        got_copy(j).start()

    dx[...] = jnp.zeros_like(dx)

    arrived(0, slot(0, 1, 0), tb)
    gather(3, slot(0, 1, 0), slot(1, 1, 0), tb, up)
    gather(4, slot(0, 1, 0), slot(2, 1, 0), tb, down)
    to_core(1, 0, 1)
    arrived(1, slot(1, 0, 0), tb)
    gather(5, slot(1, 0, 0), slot(3, 0, 0), part, up)
    to_core(2, 1, 0)
    arrived(2, slot(2, 0, 0), tb)
    gather(6, slot(2, 0, 0) + part, slot(3, 0, 0) + part, part, down)
    to_core(3, 2, 0)
    arrived(9, slot(0, 0, 1), tb)
    arrived(10, slot(0, 1, 1), tb)

    def run(stage, *which):
        for u in which:
            with jax.named_scope(f"{stage.__name__}_{u}"):
                stage(u)

    run(stage_f, 0, 1)
    run(stage_r, 0, 1)
    run(stage_a, 0, 1)
    with jax.named_scope("ag1"):
        arrived(3, slot(1, 1, 0), tb)
        gather(7, slot(1, 1, 0), slot(3, 1, 0), part, up)
        to_core(4, 1, 1)
        arrived(4, slot(2, 1, 0), tb)
        gather(8, slot(2, 1, 0) + part, slot(3, 1, 0) + part, part, down)
        to_core(5, 2, 1)
    run(stage_w, 0, 1)
    with jax.named_scope("ag2"):
        arrived(11, slot(1, 0, 1), tb)
        arrived(13, slot(1, 1, 1), tb)
        arrived(12, slot(2, 0, 1), tb)
        arrived(14, slot(2, 1, 1), tb)
    run(stage_f, 2, 3, 4, 5)
    run(stage_r, 2, 3)
    run(stage_a, 2, 3)
    run(stage_r, 4, 5)
    with jax.named_scope("ag3"):
        arrived(5, slot(3, 0, 0), part)
        arrived(6, slot(3, 0, 0) + part, part)
        to_core(6, 3, 0)
        arrived(7, slot(3, 1, 0), part)
        arrived(8, slot(3, 1, 0) + part, part)
        to_core(7, 3, 1)
        arrived(15, slot(3, 0, 1), tb)
        arrived(16, slot(3, 1, 1), tb)
    run(stage_f, 6, 7)
    run(stage_w, 2, 3)
    run(stage_a, 4, 5)
    run(stage_r, 6)
    run(stage_w, 4)
    run(stage_dx, 0, 1, 2, 3)

    last = chunks - 1

    def step(t, carry):
        def at(lag, fn):
            with jax.named_scope(fn.__name__):
                fn(t - lag)

        def at_end(lag, fn):
            j = unit(t - lag)[0]

            @pl.when(jnp.logical_and(t - lag >= 0, place(t - lag)[1] == 3))
            def _():
                with jax.named_scope(fn.__name__):
                    fn(j)

        at(0, stage_f)
        at(1, stage_r)
        at(2, stage_a)
        at(3, stage_w)
        at(4, stage_dx)
        at_end(4, stage_dw)
        at_end(7, stage_g)
        at_end(10, stage_e)
        return carry

    lax.fori_loop(8, units, step, 0)

    def dx_rows(b, zr, cr):
        return pl.ds(slot(b, zr, cr), tb)

    def core_copy(b):
        return remote(dxs.at[b], dxr.at[b], dxc_s.at[b], dxc_r.at[b], partner)

    def y1_copy(zr):
        return remote(dxs.at[3, zr], ybuf.at[zr], y1_s.at[zr], y1_r.at[zr], (up, down)[zr])

    def y2_copy(way, zr):
        return remote(
            dxs.at[2 - way, zr], y2.at[way, zr], y2_s.at[way, zr], y2_r.at[way, zr],
            (up, down)[way],
        )

    def send_core(b):
        for zr in range(2):
            dxs[b, zr] = dx[dx_rows(b, zr, 1), :].astype(BF16)
        core_copy(b).start()

    def chip_sum(b, zr):
        return dx[dx_rows(b, zr, 0), :] + dxr[b, zr].astype(F32)

    def ring_step(way):
        b, zr = 2 - way, way
        with jax.named_scope("core_wait"):
            core_copy(b).wait()
        dxs[b, 1 - zr] = chip_sum(b, 1 - zr).astype(BF16)
        y2_copy(way, 1 - zr).start()
        with jax.named_scope("y1_wait"):
            y1_copy(zr).wait_recv()
        dxs[b, zr] = (chip_sum(b, zr) + ybuf[zr].astype(F32)).astype(BF16)
        y2_copy(way, zr).start()

    run(stage_r, units - 1)
    run(stage_a, units - 2)
    run(stage_w, units - 3)
    run(stage_dx, units - 4)
    send_core(3)
    run(stage_a, units - 1)
    run(stage_w, units - 2)
    run(stage_dx, units - 3)
    send_core(2)
    core_copy(3).wait()
    for zr in range(2):
        dxs[3, zr] = chip_sum(3, zr).astype(BF16)
        y1_copy(zr).start()
    run(stage_w, units - 1)
    run(stage_dx, units - 2)
    send_core(1)
    ring_step(0)
    ring_step(1)
    run(stage_dx, units - 1)
    send_core(0)
    run(stage_g, last - 1)
    run(stage_dw, last)
    core_copy(0).wait()
    for zr in range(2):
        dx[dx_rows(0, zr, 0), :] = chip_sum(0, zr)
    z_copy = remote(dxs.at[0, 1], zbuf, z_s.at[0], z_r.at[0], near)
    with jax.named_scope("y2_wait"):
        for way in range(2):
            y2_copy(way, 1).wait_recv()
    total = dx[dx_rows(0, 1, 0), :] + y2[0, 1].astype(F32) + y2[1, 1].astype(F32)
    dxs[0, 1] = total.astype(BF16)
    z_copy.start()
    run(stage_e, last - 2)
    for way in range(2):
        y2_copy(way, 0).wait_recv()
    dx[dx_rows(0, 0, 0), :] = (
        dx[dx_rows(0, 0, 0), :] + y2[0, 0].astype(F32) + y2[1, 0].astype(F32)
    )
    run(stage_g, last)
    run(stage_e, last - 1)
    with jax.named_scope("z_wait"):
        z_copy.wait()
    dx_out[...] = dx[dx_rows(0, 0, 0), :] + zbuf[...].astype(F32)
    run(stage_e, last)

    with jax.named_scope("end"):
        for copy in started:
            copy.wait_send()
        for u in range(units - KEEP, units):
            sent(u)
        for u in range(units):
            for way in range(2):
                a1(u, way, x).wait_send()
            a2(u, opp).wait_send()
        for j in range(chunks):
            for way in range(2):
                p1(j, way).wait_send()
                p2(j, way).wait_send()
            own_copy(j).wait()
            got_copy(j).wait()
        for zr in range(2):
            y1_copy(zr).wait_send()
            for way in range(2):
                y2_copy(way, zr).wait_send()


def combine(own, got, dx, dx_out, g_out, u_out, o_out):
    for j in range(own.shape[0]):
        for m, out in enumerate((g_out, u_out, o_out)):
            lanes = pl.ds(m * W, W)
            out[:, pl.ds(j * W, W)] = own[j, :, lanes].astype(F32) + got[j, :, lanes].astype(F32)
    dx_out[...] = dx[...]


def per_device(codes, scales, mask, cot, wg, wu, wo):
    tb, dl = codes.shape
    fl = wg.shape[1]
    chunks = fl // W
    units = 4 * chunks
    dims = (tb, dl, chunks)
    tile = tb + FOOT
    vmem = pl.BlockSpec(memory_space=pltpu.VMEM)
    hbm = pl.BlockSpec(memory_space=pl.ANY)
    dma = pltpu.SemaphoreType.DMA
    grads = jax.ShapeDtypeStruct((chunks, dl, 3 * W), BF16)
    dx, own, got = pl.pallas_call(
        functools.partial(kernel, dims),
        out_shape=(jax.ShapeDtypeStruct((tb, dl), F32), grads, grads),
        in_specs=[vmem] * 4 + [hbm] * 3,
        out_specs=(vmem, hbm, hbm),
        scratch_shapes=[
            pltpu.VMEM((16 * tb, 2 * dl), BF16),
            pltpu.VMEM((chunks, dl, 3 * W), BF16),
            pltpu.VMEM((KEEP, 4, tile, 3 * W), jnp.int16),
            pltpu.VMEM((units, tile, 3 * W), jnp.int16),
            pltpu.VMEM((units, 2, tile, 3 * W), jnp.int16),
            pltpu.VMEM((chunks, 16 * tb, 3 * W), BF16),
            pltpu.VMEM((16 * tb, dl), F32),
            pltpu.VMEM((chunks, dl, 3 * W), BF16),
            pltpu.VMEM((chunks, dl, 3 * W), BF16),
            pltpu.VMEM((chunks, 2, dl // 2, 3 * W), BF16),
            pltpu.VMEM((4, 2, tb, dl), BF16),
            pltpu.VMEM((4, 2, tb, dl), BF16),
            pltpu.VMEM((2, tb, dl), BF16),
            pltpu.VMEM((2, 2, tb, dl), BF16),
            pltpu.VMEM((tb, dl), BF16),
            dma((chunks, 3)),
            dma((17,)), dma((17,)),
            dma((units,)), dma((units,)),
            dma((units, 2)), dma((units, 2)),
            dma((units, 2)), dma((units, 2)),
            dma((units,)), dma((units,)),
            dma((chunks, 2)), dma((chunks, 2)),
            dma((chunks, 2)), dma((chunks, 2)),
            dma((chunks,)), dma((chunks,)),
            dma((4,)), dma((4,)),
            dma((2,)), dma((2,)),
            dma((2, 2)), dma((2, 2)),
            dma((1,)), dma((1,)),
        ],
        compiler_params=pltpu.CompilerParams(
            collective_id=0, has_side_effects=True, vmem_limit_bytes=67043328
        ),
        name="ffn_backward",
    )(codes, scales.T, mask[None, :], cot, wg, wu, wo)
    weight = jax.ShapeDtypeStruct((dl, fl), F32)
    steps = 8
    rows = dl // steps
    return pl.pallas_call(
        combine,
        grid=(steps,),
        out_shape=(jax.ShapeDtypeStruct((tb, dl), F32), weight, weight, weight),
        in_specs=[
            pl.BlockSpec((chunks, rows, 3 * W), lambda i: (0, i, 0)),
            pl.BlockSpec((chunks, rows, 3 * W), lambda i: (0, i, 0)),
            pl.BlockSpec((tb // steps, dl), lambda i: (i, 0)),
        ],
        out_specs=[pl.BlockSpec((tb // steps, dl), lambda i: (i, 0))]
        + [pl.BlockSpec((rows, fl), lambda i: (i, 0))] * 3,
        name="combine",
    )(own, got, dx)


def solution(mesh):
    tokens = P(("dp", "col"), "row")
    weights = P("row", "col")
    return jax.shard_map(
        per_device,
        mesh=mesh,
        in_specs=(tokens, tokens, P(("dp", "col")), tokens, weights, weights, weights),
        out_specs=(tokens, weights, weights, weights),
        check_vma=False,
    )
```

```python
import functools

import jax
import jax.numpy as jnp
from jax import lax
from jax.experimental import pallas as pl
from jax.experimental.pallas import tpu as pltpu
from jax.sharding import PartitionSpec as P

MESH = pl.DeviceIdType.MESH
ROOT = 0.7978845608028654
CUBIC = 0.044715
W = 128
KEEP = 6
FOOT = 8
F32 = jnp.float32
BF16 = jnp.bfloat16


def gelu_pair(values):
    inside = ROOT * (values + CUBIC * values * values * values)
    tangent = jnp.tanh(inside)
    activated = 0.5 * values * (1.0 + tangent)
    derivative = 0.5 * (1.0 + tangent) + 0.5 * values * (1.0 - tangent * tangent) * ROOT * (
        1.0 + 3.0 * CUBIC * values * values
    )
    return activated, derivative


def coded(part):
    most = jnp.maximum(jnp.max(jnp.abs(part), axis=0, keepdims=True), 1e-30)
    power = jnp.floor(jnp.log(most) * 1.4426950408889634) + 1.0
    units = jnp.round(part * jnp.exp2(15.0 - power))
    units = jnp.clip(units, -32767.0, 32767.0).astype(jnp.int32).astype(jnp.int16)
    foot = jnp.broadcast_to(power, (FOOT, part.shape[1])).astype(jnp.int32).astype(jnp.int16)
    return units, foot


def store_coded(tile, lanes, part):
    rows = part.shape[0]
    units, foot = coded(part)
    tile[pl.ds(0, rows), lanes] = units
    tile[pl.ds(rows, FOOT), lanes] = foot


def decoded(tile, rows, lanes):
    power = tile[pl.ds(rows, FOOT), lanes].astype(jnp.int32).astype(F32)[0:1]
    units = tile[pl.ds(0, rows), lanes].astype(jnp.int32).astype(F32)
    return units * jnp.exp2(power - 15.0)


def kernel(
    dims,
    codes, scales, mask, cot, wg, wu, wo,
    dx_out, own_out, got_out,
    sl, wc, pb, r1, r2, guh, dx, acc, dws, dwr, relay, dxs, dxr, ybuf, y2, zbuf,
    w_sem, ag_s, ag_r, rs1_s, rs1_r, rs2_s, rs2_r, a1_s, a1_r, a2_s, a2_r,
    p1_s, p1_r, p2_s, p2_r, own_sem, got_sem, dxc_s, dxc_r, y1_s, y1_r, y2_s, y2_r, z_s, z_r,
):
    tb, dl, chunks = dims
    blk = 4 * tb
    units = 4 * chunks
    x = lax.axis_index("row")
    col = lax.axis_index("col")
    dp = lax.axis_index("dp")
    core = lax.rem(col, 2)
    y = lax.rem(col // 2, 4)
    z = col // 8
    opp = lax.rem(x + 2, 4)

    def at_col(dz, dy, dc):
        zz = (1 - z) if dz else z
        cc = (1 - core) if dc else core
        return {"col": (zz * 4 + lax.rem(y + dy, 4)) * 2 + cc}

    def beside(way):
        return lax.rem(x + 1 + 2 * way, 4)

    def to_row(way):
        return {"row": beside(way)}

    partner = at_col(0, 0, 1)
    up, down = at_col(0, 1, 0), at_col(0, 3, 0)
    near = at_col(1, 0, 0)
    far = dict(near, dp=1 - dp)

    barrier = pltpu.get_barrier_semaphore()
    peers = [to_row(0), to_row(1), partner, up, down, near, far]
    for peer in peers:
        pl.semaphore_signal(barrier, inc=1, device_id=peer, device_id_type=MESH)

    def weight_copy(j, m, src):
        return pltpu.make_async_copy(
            src.at[:, pl.ds(j * W, W)], wc.at[j, :, pl.ds(m * W, W)], w_sem.at[j, m]
        )

    for j in range(chunks):
        for m, src in enumerate((wg, wu, wo)):
            weight_copy(j, m, src).start()

    nb = scales.shape[0]
    flat = jnp.concatenate(
        [scales[...].astype(F32), jnp.broadcast_to(mask[...], (8, tb)).astype(F32),
         jnp.zeros((128 - nb - 8, tb), F32)], axis=0,
    )
    tall = jnp.transpose(flat)
    for k in range(nb):
        lanes = pl.ds(k * 128, 128)
        level = (2 * codes[:, lanes] - 3).astype(F32) * tall[:, k : k + 1]
        sl[pl.ds(0, tb), lanes] = (level * 0.0625).astype(BF16)
        live = cot[:, lanes].astype(F32) * tall[:, nb : nb + 1]
        sl[pl.ds(0, tb), pl.ds(dl + k * 128, 128)] = live.astype(BF16)

    with jax.named_scope("barrier"):
        pl.semaphore_wait(barrier, len(peers))

    def remote(src, dst, s_sem, r_sem, device):
        return pltpu.make_async_remote_copy(
            src_ref=src, dst_ref=dst, send_sem=s_sem, recv_sem=r_sem,
            device_id=device, device_id_type=MESH,
        )

    def slot(b, zr, cr):
        return (b * 4 + zr * 2 + cr) * tb

    def rows(start, count):
        return sl.at[pl.ds(start, count)]

    started = []

    def gather(kind, src, dst, count, device):
        copy = remote(rows(src, count), rows(dst, count), ag_s.at[kind], ag_r.at[kind], device)
        copy.start()
        started.append(copy)

    def arrived(kind, dst, count):
        remote(rows(dst, count), rows(dst, count), ag_s.at[kind], ag_r.at[kind], partner).wait_recv()

    def to_core(kind, b, zr):
        gather(9 + kind, slot(b, zr, 0), slot(b, zr, 1), tb, partner)

    part = tb // 2
    gather(0, slot(0, 0, 0), slot(0, 1, 0), tb, near)
    gather(1, slot(0, 0, 0), slot(1, 0, 0), tb, up)
    gather(2, slot(0, 0, 0), slot(2, 0, 0), tb, down)
    to_core(0, 0, 0)
    for j in range(chunks):
        for m, src in enumerate((wg, wu, wo)):
            weight_copy(j, m, src).wait()

    def place(u):
        s = (u // 8 + 1) // 2
        k = (1 - s) * (u // 2) + s * lax.rem(u, 4)
        return (1 - s) * lax.rem(u, 2) + s * (u // 4), (1 - s) * k + s * (3 - k), k

    def unit(u):
        return place(u)[:2]

    def held(u):
        return pb.at[lax.rem(u, KEEP)]

    def grad_rows(j, b, owner):
        return guh.at[j, pl.ds(pl.multiple_of((b * 4 + owner) * tb, tb), tb)]

    def rs1(u, way):
        return remote(held(u).at[opp], r1.at[u], rs1_s.at[u], rs1_r.at[u], to_row(way))

    def rs2(u, way):
        return remote(
            held(u).at[beside(way)], r2.at[u, way], rs2_s.at[u, way], rs2_r.at[u, way], to_row(way)
        )

    def a1(u, way, owner):
        j, b = unit(u)
        ref = grad_rows(j, b, owner)
        return remote(ref, ref, a1_s.at[u, way], a1_r.at[u, way], to_row(way))

    def a2(u, owner):
        j, b = unit(u)
        ref = grad_rows(j, b, owner)
        return remote(ref, ref, a2_s.at[u], a2_r.at[u], to_row(lax.rem(b, 2)))

    def sent(u):
        rs1(u, lax.rem(unit(u)[1], 2)).wait_send()
        for way in range(2):
            rs2(u, way).wait_send()

    def stage_f(u):
        j, b = unit(u)
        if isinstance(u, int):
            if u >= KEEP:
                sent(u - KEEP)
        else:
            sent(u - KEEP)
        where = pl.ds(pl.multiple_of(b * blk, blk), blk)
        both = jnp.dot(
            sl[where, pl.ds(0, dl)], wc[j, :, pl.ds(0, 2 * W)], preferred_element_type=F32
        )
        back = jnp.dot(
            sl[where, pl.ds(dl, dl)], wc[j, :, pl.ds(2 * W, W)], preferred_element_type=F32
        )
        for o in range(4):
            tile = held(u).at[o]
            store_coded(tile, pl.ds(0, 2 * W), both[o * tb : (o + 1) * tb])
            store_coded(tile, pl.ds(2 * W, W), back[o * tb : (o + 1) * tb])
        rs1(u, lax.rem(b, 2)).start()

    def stage_r(u):
        j, b = unit(u)
        way = lax.rem(b, 2)
        rs2(u, 1 - way).start()
        with jax.named_scope("r_wait"):
            rs1(u, way).wait_recv()
        tile = held(u).at[beside(way)]
        for m in range(3):
            lanes = pl.ds(m * W, W)
            total = decoded(tile, tb, lanes) + decoded(r1.at[u], tb, lanes)
            store_coded(tile, lanes, total)
        rs2(u, way).start()

    def stage_a(u):
        j, b = unit(u)
        with jax.named_scope("a_wait"):
            for way in range(2):
                rs2(u, way).wait_recv()
        tiles = (held(u).at[x], r2.at[u, 0], r2.at[u, 1])
        powers = [
            [
                jnp.exp2(t[pl.ds(tb, FOOT), pl.ds(m * W, W)].astype(jnp.int32).astype(F32)[0:1] - 15.0)
                for t in tiles
            ]
            for m in range(3)
        ]
        step = tb // 2

        def body(k, carry):
            some = pl.ds(pl.multiple_of(k * step, step), step)
            sums = []
            for m in range(3):
                total = None
                for t, power in zip(tiles, powers[m]):
                    term = t[some, pl.ds(m * W, W)].astype(jnp.int32).astype(F32) * power
                    total = term if total is None else total + term
                sums.append(total)
            gate, up_part, back = sums
            activated, derivative = gelu_pair(gate)
            to = pl.ds(pl.multiple_of((b * 4 + x) * tb + k * step, step), step)
            guh[j, to, pl.ds(0, W)] = (back * up_part * derivative).astype(BF16)
            guh[j, to, pl.ds(W, W)] = (back * activated).astype(BF16)
            guh[j, to, pl.ds(2 * W, W)] = (activated * up_part).astype(BF16)
            return carry

        lax.fori_loop(0, 2, body, 0)
        for way in range(2):
            a1(u, way, x).start()

    def stage_w(u):
        b = unit(u)[1]
        way = lax.rem(b, 2)
        with jax.named_scope("w_wait"):
            a1(u, way, beside(1 - way)).wait_recv()
        a2(u, beside(1 - way)).start()

    def arrive_dx(u):
        j, b = unit(u)
        way = lax.rem(b, 2)
        with jax.named_scope("b_wait"):
            a1(u, 1 - way, beside(way)).wait_recv()
            a2(u, opp).wait_recv()

    def add_dx(u):
        j, b = unit(u)
        where = pl.ds(pl.multiple_of(b * blk, blk), blk)
        more = lax.dot_general(
            guh[j, where, pl.ds(0, 2 * W)], wc[j, :, pl.ds(0, 2 * W)],
            (((1,), (1,)), ((), ())), preferred_element_type=F32,
        )
        dx[where, :] = dx[where, :] + more

    def stage_dx(u):
        arrive_dx(u)
        add_dx(u)

    quarter = dl // 4

    def to_z(other):
        return dict(near, dp=dp + other * (1 - 2 * dp))

    def piece(k):
        return pl.ds(pl.multiple_of(k * quarter, quarter), quarter)

    def p1(j, k):
        return remote(
            dws.at[j, piece(k)], relay.at[j, piece(k)], p1_s.at[j, k], p1_r.at[j, k], to_z(k // 2)
        )

    def p2(j, k):
        return remote(
            relay.at[j, piece(k)], dwr.at[j, piece(k)], p2_s.at[j, k], p2_r.at[j, k],
            to_z(1 - k // 2),
        )

    def own_copy(j):
        return pltpu.make_async_copy(dws.at[j], own_out.at[j], own_sem.at[j])

    def got_copy(j):
        return pltpu.make_async_copy(dwr.at[j], got_out.at[j], got_sem.at[j])

    def stage_dw(u):
        j, b, k = place(u)
        where = pl.ds(pl.multiple_of(b * blk, blk), blk)
        sums = acc.at[lax.rem(j, 2)]

        def body(i, carry):
            q = lax.rem(i, 2) * 2 + i // 2
            some = lax.dot_general(
                sl[where, piece(q)], guh[j, where, pl.ds(0, 2 * W)],
                (((0,), (0,)), ((), ())), preferred_element_type=F32,
            )
            more = lax.dot_general(
                sl[where, pl.ds(pl.multiple_of(dl + q * quarter, quarter), quarter)],
                guh[j, where, pl.ds(2 * W, W)],
                (((0,), (0,)), ((), ())), preferred_element_type=F32,
            )
            sums[piece(q), pl.ds(0, 2 * W)] = sums[piece(q), pl.ds(0, 2 * W)] + some
            sums[piece(q), pl.ds(2 * W, W)] = sums[piece(q), pl.ds(2 * W, W)] + more

            @pl.when(k == 3)
            def _():
                dws[j, piece(q), :] = sums[piece(q), :].astype(BF16)
                sums[piece(q), :] = jnp.zeros((quarter, 3 * W), F32)
                p1(j, q).start()

            return carry

        lax.fori_loop(0, 4, body, 0)

        @pl.when(k == 3)
        def _():
            own_copy(j).start()

    def stage_g(j):
        for k in (0, 2, 1, 3):
            with jax.named_scope("g_wait"):
                p1(j, k).wait_recv()
            p2(j, k).start()

    def stage_e(j):
        with jax.named_scope("e_wait"):
            for k in (0, 2, 1, 3):
                p2(j, k).wait_recv()
        got_copy(j).start()

    dx[...] = jnp.zeros_like(dx)
    acc[...] = jnp.zeros_like(acc)

    arrived(0, slot(0, 1, 0), tb)
    gather(3, slot(0, 1, 0), slot(1, 1, 0), tb, up)
    gather(4, slot(0, 1, 0), slot(2, 1, 0), tb, down)
    to_core(1, 0, 1)
    arrived(1, slot(1, 0, 0), tb)
    gather(5, slot(1, 0, 0), slot(3, 0, 0), part, up)
    to_core(2, 1, 0)
    arrived(2, slot(2, 0, 0), tb)
    gather(6, slot(2, 0, 0) + part, slot(3, 0, 0) + part, part, down)
    to_core(3, 2, 0)
    arrived(9, slot(0, 0, 1), tb)
    arrived(10, slot(0, 1, 1), tb)

    def run(stage, *which):
        for u in which:
            with jax.named_scope(f"{stage.__name__}_{u}"):
                stage(u)

    run(stage_f, 0, 1)
    run(stage_r, 0, 1)
    with jax.named_scope("ag1"):
        arrived(3, slot(1, 1, 0), tb)
        gather(7, slot(1, 1, 0), slot(3, 1, 0), part, up)
        to_core(4, 1, 1)
        arrived(4, slot(2, 1, 0), tb)
        gather(8, slot(2, 1, 0) + part, slot(3, 1, 0) + part, part, down)
        to_core(5, 2, 1)
    run(stage_a, 0, 1)
    with jax.named_scope("ag2"):
        arrived(11, slot(1, 0, 1), tb)
        arrived(13, slot(1, 1, 1), tb)
        arrived(12, slot(2, 0, 1), tb)
        arrived(14, slot(2, 1, 1), tb)
    run(stage_f, 2, 3)
    run(stage_w, 0, 1)
    run(stage_f, 4, 5)
    run(stage_r, 2, 3)
    run(stage_dx, 0)
    run(stage_dw, 0)
    run(stage_a, 2)
    run(stage_r, 4)
    run(stage_a, 3)
    run(stage_r, 5)
    run(stage_w, 2)
    with jax.named_scope("ag3"):
        arrived(5, slot(3, 0, 0), part)
        arrived(6, slot(3, 0, 0) + part, part)
        to_core(6, 3, 0)
        arrived(7, slot(3, 1, 0), part)
        arrived(8, slot(3, 1, 0) + part, part)
        to_core(7, 3, 1)
        arrived(15, slot(3, 0, 1), tb)
        arrived(16, slot(3, 1, 1), tb)
    run(stage_f, 6, 7)
    run(stage_a, 4)
    run(stage_w, 3)
    run(stage_r, 6)
    run(stage_a, 5)
    run(stage_dx, 1)
    run(stage_dw, 1)
    run(stage_w, 4)
    for u in (2, 3):
        run(stage_dx, u)
        run(stage_dw, u)

    last = chunks - 1

    def step(t, carry):
        def at(lag, fn):
            with jax.named_scope(fn.__name__):
                fn(t - lag)

        def at_end(lag, fn):
            j, b, k = place(t - lag)

            @pl.when(k == 3)
            def _():
                with jax.named_scope(fn.__name__):
                    fn(j)

        at(0, stage_f)
        at(1, stage_r)
        at(2, stage_a)
        at(3, stage_w)
        at(4, stage_dx)
        at(4, stage_dw)

        @pl.when(t >= 13)
        def _():
            at_end(7, stage_g)

        @pl.when(t >= 16)
        def _():
            at_end(10, stage_e)

        return carry

    lax.fori_loop(8, units, step, 0)

    def dx_rows(b, zr, cr):
        return pl.ds(slot(b, zr, cr), tb)

    def core_copy(b):
        return remote(dxs.at[b], dxr.at[b], dxc_s.at[b], dxc_r.at[b], partner)

    def y1_copy(zr):
        return remote(dxs.at[3, zr], ybuf.at[zr], y1_s.at[zr], y1_r.at[zr], (up, down)[zr])

    def y2_copy(way, zr):
        return remote(
            dxs.at[2 - way, zr], y2.at[way, zr], y2_s.at[way, zr], y2_r.at[way, zr],
            (up, down)[way],
        )

    def send_core(b):
        for zr in range(2):
            dxs[b, zr] = dx[dx_rows(b, zr, 1), :].astype(BF16)
        core_copy(b).start()

    def chip_sum(b, zr):
        return dx[dx_rows(b, zr, 0), :] + dxr[b, zr].astype(F32)

    def ring_early(way):
        b, zr = 2 - way, 1 - way
        with jax.named_scope("core_wait"):
            core_copy(b).wait()
        dxs[b, zr] = chip_sum(b, zr).astype(BF16)
        y2_copy(way, zr).start()

    def ring_late(way):
        b, zr = 2 - way, way
        with jax.named_scope("y1_wait"):
            y1_copy(zr).wait_recv()
        dxs[b, zr] = (chip_sum(b, zr) + ybuf[zr].astype(F32)).astype(BF16)
        y2_copy(way, zr).start()

    run(stage_r, units - 1)
    run(stage_a, units - 2)
    run(stage_w, units - 3)
    run(stage_dx, units - 4)
    send_core(3)
    run(stage_dw, units - 4)
    run(stage_a, units - 1)
    run(stage_w, units - 2)
    core_copy(3).wait()
    for zr in range(2):
        dxs[3, zr] = chip_sum(3, zr).astype(BF16)
        y1_copy(zr).start()
    run(stage_g, last - 1)
    run(stage_dx, units - 3)
    send_core(2)
    run(stage_dw, units - 3)
    run(stage_w, units - 1)
    ring_early(0)
    run(stage_dx, units - 2)
    send_core(1)
    run(stage_dw, units - 2)
    run(arrive_dx, units - 1)
    run(stage_dw, units - 1)
    ring_early(1)
    ring_late(0)
    ring_late(1)
    run(add_dx, units - 1)
    send_core(0)
    core_copy(0).wait()
    for zr in range(2):
        dx[dx_rows(0, zr, 0), :] = chip_sum(0, zr)
    z_copy = remote(dxs.at[0, 1], zbuf, z_s.at[0], z_r.at[0], near)
    with jax.named_scope("y2_wait"):
        for way in range(2):
            y2_copy(way, 1).wait_recv()
    total = dx[dx_rows(0, 1, 0), :] + y2[0, 1].astype(F32) + y2[1, 1].astype(F32)
    dxs[0, 1] = total.astype(BF16)
    z_copy.start()
    run(stage_e, last - 2)
    for way in range(2):
        y2_copy(way, 0).wait_recv()
    dx[dx_rows(0, 0, 0), :] = (
        dx[dx_rows(0, 0, 0), :] + y2[0, 0].astype(F32) + y2[1, 0].astype(F32)
    )
    run(stage_g, last)
    run(stage_e, last - 1)
    with jax.named_scope("z_wait"):
        z_copy.wait()
    dx_out[...] = dx[dx_rows(0, 0, 0), :] + zbuf[...].astype(F32)
    run(stage_e, last)

    with jax.named_scope("end"):
        for copy in started:
            copy.wait_send()
        for u in range(units - KEEP, units):
            sent(u)
        for u in range(units):
            for way in range(2):
                a1(u, way, x).wait_send()
            a2(u, opp).wait_send()
        for j in range(chunks):
            for k in range(4):
                p1(j, k).wait_send()
                p2(j, k).wait_send()
            own_copy(j).wait()
            got_copy(j).wait()
        for zr in range(2):
            y1_copy(zr).wait_send()
            for way in range(2):
                y2_copy(way, zr).wait_send()


def combine(own, got, dx, dx_out, g_out, u_out, o_out):
    for j in range(own.shape[0]):
        for m, out in enumerate((g_out, u_out, o_out)):
            lanes = pl.ds(m * W, W)
            out[:, pl.ds(j * W, W)] = own[j, :, lanes].astype(F32) + got[j, :, lanes].astype(F32)
    dx_out[...] = dx[...]


def per_device(codes, scales, mask, cot, wg, wu, wo):
    tb, dl = codes.shape
    fl = wg.shape[1]
    chunks = fl // W
    units = 4 * chunks
    dims = (tb, dl, chunks)
    tile = tb + FOOT
    vmem = pl.BlockSpec(memory_space=pltpu.VMEM)
    hbm = pl.BlockSpec(memory_space=pl.ANY)
    dma = pltpu.SemaphoreType.DMA
    grads = jax.ShapeDtypeStruct((chunks, dl, 3 * W), BF16)
    dx, own, got = pl.pallas_call(
        functools.partial(kernel, dims),
        out_shape=(jax.ShapeDtypeStruct((tb, dl), F32), grads, grads),
        in_specs=[vmem] * 4 + [hbm] * 3,
        out_specs=(vmem, hbm, hbm),
        scratch_shapes=[
            pltpu.VMEM((16 * tb, 2 * dl), BF16),
            pltpu.VMEM((chunks, dl, 3 * W), BF16),
            pltpu.VMEM((KEEP, 4, tile, 3 * W), jnp.int16),
            pltpu.VMEM((units, tile, 3 * W), jnp.int16),
            pltpu.VMEM((units, 2, tile, 3 * W), jnp.int16),
            pltpu.VMEM((chunks, 16 * tb, 3 * W), BF16),
            pltpu.VMEM((16 * tb, dl), F32),
            pltpu.VMEM((2, dl, 3 * W), F32),
            pltpu.VMEM((chunks, dl, 3 * W), BF16),
            pltpu.VMEM((chunks, dl, 3 * W), BF16),
            pltpu.VMEM((chunks, dl, 3 * W), BF16),
            pltpu.VMEM((4, 2, tb, dl), BF16),
            pltpu.VMEM((4, 2, tb, dl), BF16),
            pltpu.VMEM((2, tb, dl), BF16),
            pltpu.VMEM((2, 2, tb, dl), BF16),
            pltpu.VMEM((tb, dl), BF16),
            dma((chunks, 3)),
            dma((17,)), dma((17,)),
            dma((units,)), dma((units,)),
            dma((units, 2)), dma((units, 2)),
            dma((units, 2)), dma((units, 2)),
            dma((units,)), dma((units,)),
            dma((chunks, 4)), dma((chunks, 4)),
            dma((chunks, 4)), dma((chunks, 4)),
            dma((chunks,)), dma((chunks,)),
            dma((4,)), dma((4,)),
            dma((2,)), dma((2,)),
            dma((2, 2)), dma((2, 2)),
            dma((1,)), dma((1,)),
        ],
        compiler_params=pltpu.CompilerParams(
            collective_id=0, has_side_effects=True, vmem_limit_bytes=67043328
        ),
        name="ffn_backward",
    )(codes, scales.T, mask[None, :], cot, wg, wu, wo)
    weight = jax.ShapeDtypeStruct((dl, fl), F32)
    steps = 8
    rows = dl // steps
    return pl.pallas_call(
        combine,
        grid=(steps,),
        out_shape=(jax.ShapeDtypeStruct((tb, dl), F32), weight, weight, weight),
        in_specs=[
            pl.BlockSpec((chunks, rows, 3 * W), lambda i: (0, i, 0)),
            pl.BlockSpec((chunks, rows, 3 * W), lambda i: (0, i, 0)),
            pl.BlockSpec((tb // steps, dl), lambda i: (i, 0)),
        ],
        out_specs=[pl.BlockSpec((tb // steps, dl), lambda i: (i, 0))]
        + [pl.BlockSpec((rows, fl), lambda i: (i, 0))] * 3,
        name="combine",
    )(own, got, dx)


def solution(mesh):
    tokens = P(("dp", "col"), "row")
    weights = P("row", "col")
    return jax.shard_map(
        per_device,
        mesh=mesh,
        in_specs=(tokens, tokens, P(("dp", "col")), tokens, weights, weights, weights),
        out_specs=(tokens, weights, weights, weights),
        check_vma=False,
    )
```

```python
import functools

import jax
import jax.numpy as jnp
from jax import lax
from jax.experimental import pallas as pl
from jax.experimental.pallas import tpu as pltpu
from jax.sharding import PartitionSpec as P

MESH = pl.DeviceIdType.MESH
ROOT = 0.7978845608028654
CUBIC = 0.044715
W = 128
KEEP = 6
FOOT = 8
F32 = jnp.float32
BF16 = jnp.bfloat16


def gelu_pair(values):
    inside = ROOT * (values + CUBIC * values * values * values)
    tangent = jnp.tanh(inside)
    activated = 0.5 * values * (1.0 + tangent)
    derivative = 0.5 * (1.0 + tangent) + 0.5 * values * (1.0 - tangent * tangent) * ROOT * (
        1.0 + 3.0 * CUBIC * values * values
    )
    return activated, derivative


def coded(part):
    most = jnp.maximum(jnp.max(jnp.abs(part), axis=0, keepdims=True), 1e-30)
    power = jnp.floor(jnp.log(most) * 1.4426950408889634) + 1.0
    units = jnp.round(part * jnp.exp2(15.0 - power))
    units = jnp.clip(units, -32767.0, 32767.0).astype(jnp.int32).astype(jnp.int16)
    foot = jnp.broadcast_to(power, (FOOT, part.shape[1])).astype(jnp.int32).astype(jnp.int16)
    return units, foot


def store_coded(tile, lanes, part):
    rows = part.shape[0]
    units, foot = coded(part)
    tile[pl.ds(0, rows), lanes] = units
    tile[pl.ds(rows, FOOT), lanes] = foot


def decoded(tile, rows, lanes):
    power = tile[pl.ds(rows, FOOT), lanes].astype(jnp.int32).astype(F32)[0:1]
    units = tile[pl.ds(0, rows), lanes].astype(jnp.int32).astype(F32)
    return units * jnp.exp2(power - 15.0)


def kernel(
    dims,
    codes, scales, mask, cot, wg, wu, wo,
    dx_out, dws, dwr,
    sl, wc, pb, r1, r2, guh, dx, acc, relay, dxs, dxr, ybuf, y2, zbuf,
    w_sem, ag_s, ag_r, rs1_s, rs1_r, rs2_s, rs2_r, a1_s, a1_r, a2_s, a2_r,
    p1_s, p1_r, p2_s, p2_r, dxc_s, dxc_r, y1_s, y1_r, y2_s, y2_r, z_s, z_r,
):
    tb, dl, chunks = dims
    blk = 4 * tb
    units = 4 * chunks
    x = lax.axis_index("row")
    col = lax.axis_index("col")
    dp = lax.axis_index("dp")
    core = lax.rem(col, 2)
    y = lax.rem(col // 2, 4)
    z = col // 8
    opp = lax.rem(x + 2, 4)

    def at_col(dz, dy, dc):
        zz = (1 - z) if dz else z
        cc = (1 - core) if dc else core
        return {"col": (zz * 4 + lax.rem(y + dy, 4)) * 2 + cc}

    def beside(way):
        return lax.rem(x + 1 + 2 * way, 4)

    def to_row(way):
        return {"row": beside(way)}

    partner = at_col(0, 0, 1)
    up, down = at_col(0, 1, 0), at_col(0, 3, 0)
    near = at_col(1, 0, 0)
    far = dict(near, dp=1 - dp)

    barrier = pltpu.get_barrier_semaphore()
    peers = [to_row(0), to_row(1), partner, up, down, near, far]
    for peer in peers:
        pl.semaphore_signal(barrier, inc=1, device_id=peer, device_id_type=MESH)

    def weight_copy(j, m, src):
        return pltpu.make_async_copy(
            src.at[:, pl.ds(j * W, W)], wc.at[j, :, pl.ds(m * W, W)], w_sem.at[j, m]
        )

    for j in range(chunks):
        for m, src in enumerate((wg, wu, wo)):
            weight_copy(j, m, src).start()

    nb = scales.shape[0]
    flat = jnp.concatenate(
        [scales[...].astype(F32), jnp.broadcast_to(mask[...], (8, tb)).astype(F32),
         jnp.zeros((128 - nb - 8, tb), F32)], axis=0,
    )
    tall = jnp.transpose(flat)
    for k in range(nb):
        lanes = pl.ds(k * 128, 128)
        level = (2 * codes[:, lanes] - 3).astype(F32) * tall[:, k : k + 1]
        sl[pl.ds(0, tb), lanes] = (level * 0.0625).astype(BF16)
        live = cot[:, lanes].astype(F32) * tall[:, nb : nb + 1]
        sl[pl.ds(0, tb), pl.ds(dl + k * 128, 128)] = live.astype(BF16)

    with jax.named_scope("barrier"):
        pl.semaphore_wait(barrier, len(peers))

    def remote(src, dst, s_sem, r_sem, device):
        return pltpu.make_async_remote_copy(
            src_ref=src, dst_ref=dst, send_sem=s_sem, recv_sem=r_sem,
            device_id=device, device_id_type=MESH,
        )

    def slot(b, zr, cr):
        return (b * 4 + zr * 2 + cr) * tb

    def rows(start, count):
        return sl.at[pl.ds(start, count)]

    started = []

    def gather(kind, src, dst, count, device):
        copy = remote(rows(src, count), rows(dst, count), ag_s.at[kind], ag_r.at[kind], device)
        copy.start()
        started.append(copy)

    def arrived(kind, dst, count):
        remote(rows(dst, count), rows(dst, count), ag_s.at[kind], ag_r.at[kind], partner).wait_recv()

    def to_core(kind, b, zr):
        gather(9 + kind, slot(b, zr, 0), slot(b, zr, 1), tb, partner)

    part = tb // 2
    gather(0, slot(0, 0, 0), slot(0, 1, 0), tb, near)
    gather(1, slot(0, 0, 0), slot(1, 0, 0), tb, up)
    gather(2, slot(0, 0, 0), slot(2, 0, 0), tb, down)
    to_core(0, 0, 0)
    for j in range(chunks):
        for m, src in enumerate((wg, wu, wo)):
            weight_copy(j, m, src).wait()

    def place(u):
        if isinstance(u, int) and u < 3:
            return u, 0, 0
        late, whole = (u + 3) // 12, u // 12
        first = (u - 3) // 2 + 1
        k = lax.rem(u, 4)
        return (
            (1 - late) * lax.rem(u - 3, 2) + late * (u // 4),
            (1 - late) * first + late * (4 - whole - k),
            (1 - late) * first + late * k,
        )

    def unit(u):
        return place(u)[:2]

    def held(u):
        return pb.at[lax.rem(u, KEEP)]

    def grad_rows(j, b, owner):
        return guh.at[j, pl.ds(pl.multiple_of((b * 4 + owner) * tb, tb), tb)]

    def rs1(u, way):
        return remote(held(u).at[opp], r1.at[u], rs1_s.at[u], rs1_r.at[u], to_row(way))

    def rs2(u, way):
        return remote(
            held(u).at[beside(way)], r2.at[u, way], rs2_s.at[u, way], rs2_r.at[u, way], to_row(way)
        )

    def a1(u, way, owner):
        j, b = unit(u)
        ref = grad_rows(j, b, owner)
        return remote(ref, ref, a1_s.at[u, way], a1_r.at[u, way], to_row(way))

    def a2(u, owner):
        j, b = unit(u)
        ref = grad_rows(j, b, owner)
        return remote(ref, ref, a2_s.at[u], a2_r.at[u], to_row(lax.rem(b, 2)))

    def sent(u):
        rs1(u, lax.rem(unit(u)[1], 2)).wait_send()
        for way in range(2):
            rs2(u, way).wait_send()

    def stage_f(u):
        j, b = unit(u)
        if isinstance(u, int):
            if u >= KEEP:
                sent(u - KEEP)
        else:
            sent(u - KEEP)
        where = pl.ds(pl.multiple_of(b * blk, blk), blk)
        both = jnp.dot(
            sl[where, pl.ds(0, dl)], wc[j, :, pl.ds(0, 2 * W)], preferred_element_type=F32
        )
        back = jnp.dot(
            sl[where, pl.ds(dl, dl)], wc[j, :, pl.ds(2 * W, W)], preferred_element_type=F32
        )
        for o in range(4):
            tile = held(u).at[o]
            store_coded(tile, pl.ds(0, 2 * W), both[o * tb : (o + 1) * tb])
            store_coded(tile, pl.ds(2 * W, W), back[o * tb : (o + 1) * tb])
        rs1(u, lax.rem(b, 2)).start()

    def stage_r(u):
        j, b = unit(u)
        way = lax.rem(b, 2)
        rs2(u, 1 - way).start()
        with jax.named_scope("r_wait"):
            rs1(u, way).wait_recv()
        tile = held(u).at[beside(way)]
        for m in range(3):
            lanes = pl.ds(m * W, W)
            total = decoded(tile, tb, lanes) + decoded(r1.at[u], tb, lanes)
            store_coded(tile, lanes, total)
        rs2(u, way).start()

    def stage_a(u):
        j, b = unit(u)
        with jax.named_scope("a_wait"):
            for way in range(2):
                rs2(u, way).wait_recv()
        tiles = (held(u).at[x], r2.at[u, 0], r2.at[u, 1])
        powers = [
            [
                jnp.exp2(t[pl.ds(tb, FOOT), pl.ds(m * W, W)].astype(jnp.int32).astype(F32)[0:1] - 15.0)
                for t in tiles
            ]
            for m in range(3)
        ]
        step = tb // 2

        def body(k, carry):
            some = pl.ds(pl.multiple_of(k * step, step), step)
            sums = []
            for m in range(3):
                total = None
                for t, power in zip(tiles, powers[m]):
                    term = t[some, pl.ds(m * W, W)].astype(jnp.int32).astype(F32) * power
                    total = term if total is None else total + term
                sums.append(total)
            gate, up_part, back = sums
            activated, derivative = gelu_pair(gate)
            to = pl.ds(pl.multiple_of((b * 4 + x) * tb + k * step, step), step)
            guh[j, to, pl.ds(0, W)] = (back * up_part * derivative).astype(BF16)
            guh[j, to, pl.ds(W, W)] = (back * activated).astype(BF16)
            guh[j, to, pl.ds(2 * W, W)] = (activated * up_part).astype(BF16)
            return carry

        lax.fori_loop(0, 2, body, 0)
        for way in range(2):
            a1(u, way, x).start()

    def stage_w(u):
        b = unit(u)[1]
        way = lax.rem(b, 2)
        with jax.named_scope("w_wait"):
            a1(u, way, beside(1 - way)).wait_recv()
        a2(u, beside(1 - way)).start()

    def arrive_dx(u):
        j, b = unit(u)
        way = lax.rem(b, 2)
        with jax.named_scope("b_wait"):
            a1(u, 1 - way, beside(way)).wait_recv()
            a2(u, opp).wait_recv()

    def add_dx(u):
        j, b = unit(u)
        where = pl.ds(pl.multiple_of(b * blk, blk), blk)
        more = lax.dot_general(
            guh[j, where, pl.ds(0, 2 * W)], wc[j, :, pl.ds(0, 2 * W)],
            (((1,), (1,)), ((), ())), preferred_element_type=F32,
        )
        dx[where, :] = dx[where, :] + more

    def stage_dx(u):
        arrive_dx(u)
        add_dx(u)

    quarter = dl // 4

    def to_z(other):
        return dict(near, dp=dp + other * (1 - 2 * dp))

    def piece(k):
        return pl.ds(pl.multiple_of(k * quarter, quarter), quarter)

    def p1(j, k):
        return remote(
            dws.at[j, piece(k)], relay.at[j, piece(k)], p1_s.at[j, k], p1_r.at[j, k], to_z(k // 2)
        )

    def p2(j, k):
        return remote(
            relay.at[j, piece(k)], dwr.at[j, piece(k)], p2_s.at[j, k], p2_r.at[j, k],
            to_z(1 - k // 2),
        )

    def stage_dw(u):
        j, b, k = place(u)
        where = pl.ds(pl.multiple_of(b * blk, blk), blk)
        sums = acc.at[lax.rem(j, 3)]

        def body(i, carry):
            q = lax.rem(i, 2) * 2 + i // 2
            some = lax.dot_general(
                sl[where, piece(q)], guh[j, where, pl.ds(0, 2 * W)],
                (((0,), (0,)), ((), ())), preferred_element_type=F32,
            )
            more = lax.dot_general(
                sl[where, pl.ds(pl.multiple_of(dl + q * quarter, quarter), quarter)],
                guh[j, where, pl.ds(2 * W, W)],
                (((0,), (0,)), ((), ())), preferred_element_type=F32,
            )
            sums[piece(q), pl.ds(0, 2 * W)] = sums[piece(q), pl.ds(0, 2 * W)] + some
            sums[piece(q), pl.ds(2 * W, W)] = sums[piece(q), pl.ds(2 * W, W)] + more

            @pl.when(k == 3)
            def _():
                dws[j, piece(q), :] = sums[piece(q), :].astype(BF16)
                sums[piece(q), :] = jnp.zeros((quarter, 3 * W), F32)
                p1(j, q).start()

            return carry

        lax.fori_loop(0, 4, body, 0)

    def stage_g(j):
        for k in (0, 2, 1, 3):
            with jax.named_scope("g_wait"):
                p1(j, k).wait_recv()
            p2(j, k).start()

    def stage_e(j):
        with jax.named_scope("e_wait"):
            for k in (0, 2, 1, 3):
                p2(j, k).wait_recv()

    dx[...] = jnp.zeros_like(dx)
    acc[...] = jnp.zeros_like(acc)

    arrived(0, slot(0, 1, 0), tb)
    gather(3, slot(0, 1, 0), slot(1, 1, 0), tb, up)
    gather(4, slot(0, 1, 0), slot(2, 1, 0), tb, down)
    to_core(1, 0, 1)
    arrived(1, slot(1, 0, 0), tb)
    gather(5, slot(1, 0, 0), slot(3, 0, 0), part, up)
    to_core(2, 1, 0)
    arrived(2, slot(2, 0, 0), tb)
    gather(6, slot(2, 0, 0) + part, slot(3, 0, 0) + part, part, down)
    to_core(3, 2, 0)
    arrived(9, slot(0, 0, 1), tb)
    arrived(10, slot(0, 1, 1), tb)

    def run(stage, *which):
        for u in which:
            with jax.named_scope(f"{stage.__name__}_{u}"):
                stage(u)

    def finish(u):
        run(stage_dx, u)
        run(stage_dw, u)

    run(stage_f, 0, 1, 2)
    run(stage_r, 0, 1, 2)
    run(stage_a, 0)
    with jax.named_scope("ag1"):
        arrived(3, slot(1, 1, 0), tb)
        gather(7, slot(1, 1, 0), slot(3, 1, 0), part, up)
        to_core(4, 1, 1)
        arrived(4, slot(2, 1, 0), tb)
        gather(8, slot(2, 1, 0) + part, slot(3, 1, 0) + part, part, down)
        to_core(5, 2, 1)
    run(stage_a, 1)
    with jax.named_scope("ag2"):
        arrived(11, slot(1, 0, 1), tb)
        arrived(13, slot(1, 1, 1), tb)
        arrived(12, slot(2, 0, 1), tb)
        arrived(14, slot(2, 1, 1), tb)
    run(stage_f, 3, 4, 5, 6)
    run(stage_a, 2)
    run(stage_w, 0, 1)
    run(stage_r, 3, 4)
    run(stage_w, 2)
    finish(0)
    finish(1)
    run(stage_a, 3)
    run(stage_r, 5)
    run(stage_a, 4)
    run(stage_w, 3)
    with jax.named_scope("ag3"):
        arrived(5, slot(3, 0, 0), part)
        arrived(6, slot(3, 0, 0) + part, part)
        to_core(6, 3, 0)
        arrived(7, slot(3, 1, 0), part)
        arrived(8, slot(3, 1, 0) + part, part)
        to_core(7, 3, 1)
        arrived(15, slot(3, 0, 1), tb)
        arrived(16, slot(3, 1, 1), tb)
    run(stage_f, 7)
    run(stage_r, 6)
    finish(2)
    run(stage_a, 5)
    run(stage_w, 4)
    finish(3)

    last = chunks - 1

    def step(t, carry):
        def at(lag, fn):
            with jax.named_scope(fn.__name__):
                fn(t - lag)

        def at_end(lag, fn):
            j, b, k = place(t - lag)

            @pl.when(k == 3)
            def _():
                with jax.named_scope(fn.__name__):
                    fn(j)

        at(0, stage_f)
        at(1, stage_r)
        at(2, stage_a)
        at(3, stage_w)
        at(4, stage_dx)
        at(4, stage_dw)

        @pl.when(t >= 14)
        def _():
            at_end(7, stage_g)

        @pl.when(t >= 17)
        def _():
            at_end(10, stage_e)

        return carry

    lax.fori_loop(8, units, step, 0)

    def dx_rows(b, zr, cr):
        return pl.ds(slot(b, zr, cr), tb)

    def core_copy(b):
        return remote(dxs.at[b], dxr.at[b], dxc_s.at[b], dxc_r.at[b], partner)

    def y1_copy(zr):
        return remote(dxs.at[3, zr], ybuf.at[zr], y1_s.at[zr], y1_r.at[zr], (up, down)[zr])

    def y2_copy(way, zr):
        return remote(
            dxs.at[2 - way, zr], y2.at[way, zr], y2_s.at[way, zr], y2_r.at[way, zr],
            (up, down)[way],
        )

    def send_core(b):
        for zr in range(2):
            dxs[b, zr] = dx[dx_rows(b, zr, 1), :].astype(BF16)
        core_copy(b).start()

    def chip_sum(b, zr):
        return dx[dx_rows(b, zr, 0), :] + dxr[b, zr].astype(F32)

    def ring_early(way):
        b, zr = 2 - way, 1 - way
        if way == 0:
            with jax.named_scope("core_wait"):
                core_copy(b).wait()
        dxs[b, zr] = chip_sum(b, zr).astype(BF16)
        y2_copy(way, zr).start()

    def ring_late(way):
        b, zr = 2 - way, way
        if way == 1:
            with jax.named_scope("core_wait"):
                core_copy(b).wait()
        with jax.named_scope("y1_wait"):
            y1_copy(zr).wait_recv()
        dxs[b, zr] = (chip_sum(b, zr) + ybuf[zr].astype(F32)).astype(BF16)
        y2_copy(way, zr).start()

    run(stage_r, units - 1)
    run(stage_a, units - 2)
    run(stage_w, units - 3)
    run(stage_dx, units - 4)
    send_core(3)
    run(stage_a, units - 1)
    run(stage_w, units - 2)
    run(stage_dw, units - 4)
    core_copy(3).wait()
    for zr in range(2):
        dxs[3, zr] = chip_sum(3, zr).astype(BF16)
        y1_copy(zr).start()
    run(stage_dx, units - 3)
    send_core(2)
    run(stage_dw, units - 3)
    run(stage_w, units - 1)
    run(stage_g, last - 1)
    run(stage_dx, units - 2)
    send_core(1)
    ring_early(0)
    run(stage_dw, units - 2)
    ring_late(1)
    run(arrive_dx, units - 1)
    run(stage_dw, units - 1)
    ring_early(1)
    ring_late(0)
    run(add_dx, units - 1)
    send_core(0)
    core_copy(0).wait()
    for zr in range(2):
        dx[dx_rows(0, zr, 0), :] = chip_sum(0, zr)
    z_copy = remote(dxs.at[0, 1], zbuf, z_s.at[0], z_r.at[0], near)
    with jax.named_scope("y2_wait"):
        for way in range(2):
            y2_copy(way, 1).wait_recv()
    total = dx[dx_rows(0, 1, 0), :] + y2[0, 1].astype(F32) + y2[1, 1].astype(F32)
    dxs[0, 1] = total.astype(BF16)
    z_copy.start()
    with jax.named_scope("g_last"):
        stage_g(last)
    with jax.named_scope("y2_wait"):
        for way in range(2):
            y2_copy(way, 0).wait_recv()
    dx[dx_rows(0, 0, 0), :] = (
        dx[dx_rows(0, 0, 0), :] + y2[0, 0].astype(F32) + y2[1, 0].astype(F32)
    )
    run(stage_e, last - 2)
    run(stage_e, last - 1)
    with jax.named_scope("z_wait"):
        z_copy.wait()
    dx_out[...] = dx[dx_rows(0, 0, 0), :] + zbuf[...].astype(F32)
    run(stage_e, last)

    with jax.named_scope("end"):
        for copy in started:
            copy.wait_send()
        for u in range(units - KEEP, units):
            sent(u)
        for u in range(units):
            for way in range(2):
                a1(u, way, x).wait_send()
            a2(u, opp).wait_send()
        for j in range(chunks):
            for k in range(4):
                p1(j, k).wait_send()
                p2(j, k).wait_send()
        for zr in range(2):
            y1_copy(zr).wait_send()
            for way in range(2):
                y2_copy(way, zr).wait_send()


def combine(own, got, dx, dx_out, g_out, u_out, o_out):
    rows = g_out.shape[0]
    where = pl.ds(pl.multiple_of(pl.program_id(0) * rows, rows), rows)
    for j in range(own.shape[0]):
        for m, out in enumerate((g_out, u_out, o_out)):
            lanes = pl.ds(m * W, W)
            total = own[j, where, lanes].astype(F32) + got[j, where, lanes].astype(F32)
            out[:, pl.ds(j * W, W)] = total
    some = dx_out.shape[0]
    dx_out[...] = dx[pl.ds(pl.multiple_of(pl.program_id(0) * some, some), some), :]


def per_device(codes, scales, mask, cot, wg, wu, wo):
    tb, dl = codes.shape
    fl = wg.shape[1]
    chunks = fl // W
    units = 4 * chunks
    dims = (tb, dl, chunks)
    tile = tb + FOOT
    vmem = pl.BlockSpec(memory_space=pltpu.VMEM)
    hbm = pl.BlockSpec(memory_space=pl.ANY)
    dma = pltpu.SemaphoreType.DMA
    grads = pltpu.VMEM((chunks, dl, 3 * W), BF16)
    dx, own, got = pl.pallas_call(
        functools.partial(kernel, dims),
        out_shape=(pltpu.VMEM((tb, dl), F32), grads, grads),
        in_specs=[vmem] * 4 + [hbm] * 3,
        out_specs=(vmem, vmem, vmem),
        scratch_shapes=[
            pltpu.VMEM((16 * tb, 2 * dl), BF16),
            pltpu.VMEM((chunks, dl, 3 * W), BF16),
            pltpu.VMEM((KEEP, 4, tile, 3 * W), jnp.int16),
            pltpu.VMEM((units, tile, 3 * W), jnp.int16),
            pltpu.VMEM((units, 2, tile, 3 * W), jnp.int16),
            pltpu.VMEM((chunks, 16 * tb, 3 * W), BF16),
            pltpu.VMEM((16 * tb, dl), F32),
            pltpu.VMEM((3, dl, 3 * W), F32),
            pltpu.VMEM((chunks, dl, 3 * W), BF16),
            pltpu.VMEM((4, 2, tb, dl), BF16),
            pltpu.VMEM((4, 2, tb, dl), BF16),
            pltpu.VMEM((2, tb, dl), BF16),
            pltpu.VMEM((2, 2, tb, dl), BF16),
            pltpu.VMEM((tb, dl), BF16),
            dma((chunks, 3)),
            dma((17,)), dma((17,)),
            dma((units,)), dma((units,)),
            dma((units, 2)), dma((units, 2)),
            dma((units, 2)), dma((units, 2)),
            dma((units,)), dma((units,)),
            dma((chunks, 4)), dma((chunks, 4)),
            dma((chunks, 4)), dma((chunks, 4)),
            dma((4,)), dma((4,)),
            dma((2,)), dma((2,)),
            dma((2, 2)), dma((2, 2)),
            dma((1,)), dma((1,)),
        ],
        compiler_params=pltpu.CompilerParams(
            collective_id=0, has_side_effects=True, vmem_limit_bytes=57671680
        ),
        name="ffn_backward",
    )(codes, scales.T, mask[None, :], cot, wg, wu, wo)
    weight = jax.ShapeDtypeStruct((dl, fl), F32)
    steps = 8
    rows = dl // steps
    return pl.pallas_call(
        combine,
        grid=(steps,),
        out_shape=(jax.ShapeDtypeStruct((tb, dl), F32), weight, weight, weight),
        in_specs=[vmem] * 3,
        out_specs=[pl.BlockSpec((tb // steps, dl), lambda i: (i, 0))]
        + [pl.BlockSpec((rows, fl), lambda i: (i, 0))] * 3,
        compiler_params=pltpu.CompilerParams(vmem_limit_bytes=24 * 1024 * 1024),
        name="combine",
    )(own, got, dx)


def solution(mesh):
    tokens = P(("dp", "col"), "row")
    weights = P("row", "col")
    return jax.shard_map(
        per_device,
        mesh=mesh,
        in_specs=(tokens, tokens, P(("dp", "col")), tokens, weights, weights, weights),
        out_specs=(tokens, weights, weights, weights),
        check_vma=False,
    )
```

```python
import functools

import jax
import jax.numpy as jnp
from jax import lax
from jax.experimental import pallas as pl
from jax.experimental.pallas import tpu as pltpu
from jax.sharding import PartitionSpec as P

MESH = pl.DeviceIdType.MESH
ROOT = 0.7978845608028654
CUBIC = 0.044715
W = 128
KEEP = 6
FOOT = 8
F32 = jnp.float32
BF16 = jnp.bfloat16


def gelu_pair(values):
    inside = ROOT * (values + CUBIC * values * values * values)
    tangent = jnp.tanh(inside)
    activated = 0.5 * values * (1.0 + tangent)
    derivative = 0.5 * (1.0 + tangent) + 0.5 * values * (1.0 - tangent * tangent) * ROOT * (
        1.0 + 3.0 * CUBIC * values * values
    )
    return activated, derivative


def coded(part):
    most = jnp.maximum(jnp.max(jnp.abs(part), axis=0, keepdims=True), 1e-30)
    power = jnp.floor(jnp.log(most) * 1.4426950408889634) + 1.0
    units = jnp.round(part * jnp.exp2(15.0 - power))
    units = jnp.clip(units, -32767.0, 32767.0).astype(jnp.int32).astype(jnp.int16)
    foot = jnp.broadcast_to(power, (FOOT, part.shape[1])).astype(jnp.int32).astype(jnp.int16)
    return units, foot


def store_coded(tile, lanes, part):
    rows = part.shape[0]
    units, foot = coded(part)
    tile[pl.ds(0, rows), lanes] = units
    tile[pl.ds(rows, FOOT), lanes] = foot


def decoded(tile, rows, lanes):
    power = tile[pl.ds(rows, FOOT), lanes].astype(jnp.int32).astype(F32)[0:1]
    units = tile[pl.ds(0, rows), lanes].astype(jnp.int32).astype(F32)
    return units * jnp.exp2(power - 15.0)


def kernel(
    dims,
    codes, scales, mask, cot, wg, wu, wo,
    dx_out, dws, dwr,
    sl, wc, pb, r1, r2, guh, dx, acc, relay, dxs, dxr, ybuf, y2, zbuf,
    w_sem, ag_s, ag_r, rs1_s, rs1_r, rs2_s, rs2_r, a1_s, a1_r, a2_s, a2_r,
    p1_s, p1_r, p2_s, p2_r, dxc_s, dxc_r, y1_s, y1_r, y2_s, y2_r, z_s, z_r,
):
    tb, dl, chunks = dims
    blk = 4 * tb
    units = 4 * chunks
    x = lax.axis_index("row")
    col = lax.axis_index("col")
    dp = lax.axis_index("dp")
    core = lax.rem(col, 2)
    y = lax.rem(col // 2, 4)
    z = col // 8
    opp = lax.rem(x + 2, 4)

    def at_col(dz, dy, dc):
        zz = (1 - z) if dz else z
        cc = (1 - core) if dc else core
        return {"col": (zz * 4 + lax.rem(y + dy, 4)) * 2 + cc}

    def beside(way):
        return lax.rem(x + 1 + 2 * way, 4)

    def to_row(way):
        return {"row": beside(way)}

    partner = at_col(0, 0, 1)
    up, down = at_col(0, 1, 0), at_col(0, 3, 0)
    near = at_col(1, 0, 0)
    far = dict(near, dp=1 - dp)

    barrier = pltpu.get_barrier_semaphore()
    peers = [to_row(0), to_row(1), partner, up, down, near, far]
    for peer in peers:
        pl.semaphore_signal(barrier, inc=1, device_id=peer, device_id_type=MESH)

    def weight_copy(j, m, src):
        return pltpu.make_async_copy(
            src.at[:, pl.ds(j * W, W)], wc.at[j, :, pl.ds(m * W, W)], w_sem.at[j, m]
        )

    for j in range(chunks):
        for m, src in enumerate((wg, wu, wo)):
            weight_copy(j, m, src).start()

    nb = scales.shape[0]
    flat = jnp.concatenate(
        [scales[...].astype(F32), jnp.broadcast_to(mask[...], (8, tb)).astype(F32),
         jnp.zeros((128 - nb - 8, tb), F32)], axis=0,
    )
    tall = jnp.transpose(flat)
    for k in range(nb):
        lanes = pl.ds(k * 128, 128)
        level = (2 * codes[:, lanes] - 3).astype(F32) * tall[:, k : k + 1]
        sl[pl.ds(0, tb), lanes] = (level * 0.0625).astype(BF16)
        live = cot[:, lanes].astype(F32) * tall[:, nb : nb + 1]
        sl[pl.ds(0, tb), pl.ds(dl + k * 128, 128)] = live.astype(BF16)

    with jax.named_scope("barrier"):
        pl.semaphore_wait(barrier, len(peers))

    def remote(src, dst, s_sem, r_sem, device):
        return pltpu.make_async_remote_copy(
            src_ref=src, dst_ref=dst, send_sem=s_sem, recv_sem=r_sem,
            device_id=device, device_id_type=MESH,
        )

    def slot(b, zr, cr):
        return (b * 4 + zr * 2 + cr) * tb

    def rows(start, count):
        return sl.at[pl.ds(start, count)]

    started = []

    def gather(kind, src, dst, count, device):
        copy = remote(rows(src, count), rows(dst, count), ag_s.at[kind], ag_r.at[kind], device)
        copy.start()
        started.append(copy)

    def arrived(kind, dst, count):
        remote(rows(dst, count), rows(dst, count), ag_s.at[kind], ag_r.at[kind], partner).wait_recv()

    def to_core(kind, b, zr):
        gather(9 + kind, slot(b, zr, 0), slot(b, zr, 1), tb, partner)

    part = tb // 2
    gather(0, slot(0, 0, 0), slot(0, 1, 0), tb, near)
    gather(1, slot(0, 0, 0), slot(1, 0, 0), tb, up)
    gather(2, slot(0, 0, 0), slot(2, 0, 0), tb, down)
    to_core(0, 0, 0)
    for j in range(chunks):
        for m, src in enumerate((wg, wu, wo)):
            weight_copy(j, m, src).wait()

    def place(u):
        if isinstance(u, int) and u < 3:
            return u, 0, 0
        late, whole = (u + 3) // 12, u // 12
        first = (u - 3) // 2 + 1
        k = lax.rem(u, 4)
        return (
            (1 - late) * lax.rem(u - 3, 2) + late * (u // 4),
            (1 - late) * first + late * (4 - whole - k),
            (1 - late) * first + late * k,
        )

    def unit(u):
        return place(u)[:2]

    def held(u):
        return pb.at[lax.rem(u, KEEP)]

    def grad_rows(j, b, owner):
        return guh.at[j, pl.ds(pl.multiple_of((b * 4 + owner) * tb, tb), tb)]

    def rs1(u, way):
        return remote(held(u).at[opp], r1.at[u], rs1_s.at[u], rs1_r.at[u], to_row(way))

    def rs2(u, way):
        return remote(
            held(u).at[beside(way)], r2.at[u, way], rs2_s.at[u, way], rs2_r.at[u, way], to_row(way)
        )

    def a1(u, way, owner):
        j, b = unit(u)
        ref = grad_rows(j, b, owner)
        return remote(ref, ref, a1_s.at[u, way], a1_r.at[u, way], to_row(way))

    def a2(u, owner):
        j, b = unit(u)
        ref = grad_rows(j, b, owner)
        return remote(ref, ref, a2_s.at[u], a2_r.at[u], to_row(lax.rem(u, 2)))

    def sent(u):
        rs1(u, lax.rem(u, 2)).wait_send()
        for way in range(2):
            rs2(u, way).wait_send()

    def stage_f(u):
        j, b = unit(u)
        if isinstance(u, int):
            if u >= KEEP:
                sent(u - KEEP)
        else:
            sent(u - KEEP)
        where = pl.ds(pl.multiple_of(b * blk, blk), blk)
        both = jnp.dot(
            sl[where, pl.ds(0, dl)], wc[j, :, pl.ds(0, 2 * W)], preferred_element_type=F32
        )
        back = jnp.dot(
            sl[where, pl.ds(dl, dl)], wc[j, :, pl.ds(2 * W, W)], preferred_element_type=F32
        )
        for o in range(4):
            tile = held(u).at[o]
            store_coded(tile, pl.ds(0, 2 * W), both[o * tb : (o + 1) * tb])
            store_coded(tile, pl.ds(2 * W, W), back[o * tb : (o + 1) * tb])
        rs1(u, lax.rem(u, 2)).start()

    def stage_r(u):
        j, b = unit(u)
        way = lax.rem(u, 2)
        rs2(u, 1 - way).start()
        with jax.named_scope("r_wait"):
            rs1(u, way).wait_recv()
        tile = held(u).at[beside(way)]
        for m in range(3):
            lanes = pl.ds(m * W, W)
            total = decoded(tile, tb, lanes) + decoded(r1.at[u], tb, lanes)
            store_coded(tile, lanes, total)
        rs2(u, way).start()

    def stage_a(u):
        j, b = unit(u)
        with jax.named_scope("a_wait"):
            for way in range(2):
                rs2(u, way).wait_recv()
        tiles = (held(u).at[x], r2.at[u, 0], r2.at[u, 1])
        powers = [
            [
                jnp.exp2(t[pl.ds(tb, FOOT), pl.ds(m * W, W)].astype(jnp.int32).astype(F32)[0:1] - 15.0)
                for t in tiles
            ]
            for m in range(3)
        ]
        step = tb // 2

        def body(k, carry):
            some = pl.ds(pl.multiple_of(k * step, step), step)
            sums = []
            for m in range(3):
                total = None
                for t, power in zip(tiles, powers[m]):
                    term = t[some, pl.ds(m * W, W)].astype(jnp.int32).astype(F32) * power
                    total = term if total is None else total + term
                sums.append(total)
            gate, up_part, back = sums
            activated, derivative = gelu_pair(gate)
            to = pl.ds(pl.multiple_of((b * 4 + x) * tb + k * step, step), step)
            guh[j, to, pl.ds(0, W)] = (back * up_part * derivative).astype(BF16)
            guh[j, to, pl.ds(W, W)] = (back * activated).astype(BF16)
            guh[j, to, pl.ds(2 * W, W)] = (activated * up_part).astype(BF16)
            return carry

        lax.fori_loop(0, 2, body, 0)
        for way in range(2):
            a1(u, way, x).start()

    def stage_w(u):
        way = lax.rem(u, 2)
        with jax.named_scope("w_wait"):
            a1(u, way, beside(1 - way)).wait_recv()
        a2(u, beside(1 - way)).start()

    def arrive_dx(u):
        j, b = unit(u)
        way = lax.rem(u, 2)
        with jax.named_scope("b_wait"):
            a1(u, 1 - way, beside(way)).wait_recv()
            a2(u, opp).wait_recv()

    def add_dx(u):
        j, b = unit(u)
        where = pl.ds(pl.multiple_of(b * blk, blk), blk)
        more = lax.dot_general(
            guh[j, where, pl.ds(0, 2 * W)], wc[j, :, pl.ds(0, 2 * W)],
            (((1,), (1,)), ((), ())), preferred_element_type=F32,
        )
        dx[where, :] = dx[where, :] + more

    def stage_dx(u):
        arrive_dx(u)
        add_dx(u)

    quarter = dl // 4

    def to_z(other):
        return dict(near, dp=dp + other * (1 - 2 * dp))

    def piece(k):
        return pl.ds(pl.multiple_of(k * quarter, quarter), quarter)

    def p1(j, k):
        return remote(
            dws.at[j, piece(k)], relay.at[j, piece(k)], p1_s.at[j, k], p1_r.at[j, k], to_z(k // 2)
        )

    def p2(j, k):
        return remote(
            relay.at[j, piece(k)], dwr.at[j, piece(k)], p2_s.at[j, k], p2_r.at[j, k],
            to_z(1 - k // 2),
        )

    def stage_dw(u):
        j, b, k = place(u)
        where = pl.ds(pl.multiple_of(b * blk, blk), blk)
        sums = acc.at[lax.rem(j, 3)]

        def body(i, carry):
            q = lax.rem(i, 2) * 2 + i // 2
            some = lax.dot_general(
                sl[where, piece(q)], guh[j, where, pl.ds(0, 2 * W)],
                (((0,), (0,)), ((), ())), preferred_element_type=F32,
            )
            more = lax.dot_general(
                sl[where, pl.ds(pl.multiple_of(dl + q * quarter, quarter), quarter)],
                guh[j, where, pl.ds(2 * W, W)],
                (((0,), (0,)), ((), ())), preferred_element_type=F32,
            )
            sums[piece(q), pl.ds(0, 2 * W)] = sums[piece(q), pl.ds(0, 2 * W)] + some
            sums[piece(q), pl.ds(2 * W, W)] = sums[piece(q), pl.ds(2 * W, W)] + more

            @pl.when(k == 3)
            def _():
                dws[j, piece(q), :] = sums[piece(q), :].astype(BF16)
                sums[piece(q), :] = jnp.zeros((quarter, 3 * W), F32)
                p1(j, q).start()

            return carry

        lax.fori_loop(0, 4, body, 0)

    def stage_g(j):
        for k in (0, 2, 1, 3):
            with jax.named_scope("g_wait"):
                p1(j, k).wait_recv()
            p2(j, k).start()

    def stage_e(j):
        with jax.named_scope("e_wait"):
            for k in (0, 2, 1, 3):
                p2(j, k).wait_recv()

    dx[...] = jnp.zeros_like(dx)
    acc[...] = jnp.zeros_like(acc)

    arrived(0, slot(0, 1, 0), tb)
    gather(3, slot(0, 1, 0), slot(1, 1, 0), tb, up)
    gather(4, slot(0, 1, 0), slot(2, 1, 0), tb, down)
    to_core(1, 0, 1)
    arrived(1, slot(1, 0, 0), tb)
    gather(5, slot(1, 0, 0), slot(3, 0, 0), part, up)
    to_core(2, 1, 0)
    arrived(2, slot(2, 0, 0), tb)
    gather(6, slot(2, 0, 0) + part, slot(3, 0, 0) + part, part, down)
    to_core(3, 2, 0)
    arrived(9, slot(0, 0, 1), tb)
    arrived(10, slot(0, 1, 1), tb)

    def run(stage, *which):
        for u in which:
            with jax.named_scope(f"{stage.__name__}_{u}"):
                stage(u)

    def finish(u):
        run(stage_dx, u)
        run(stage_dw, u)

    run(stage_f, 0, 1, 2)
    run(stage_r, 0, 1, 2)
    run(stage_a, 0)
    with jax.named_scope("ag1"):
        arrived(3, slot(1, 1, 0), tb)
        gather(7, slot(1, 1, 0), slot(3, 1, 0), part, up)
        to_core(4, 1, 1)
        arrived(4, slot(2, 1, 0), tb)
        gather(8, slot(2, 1, 0) + part, slot(3, 1, 0) + part, part, down)
        to_core(5, 2, 1)
    run(stage_a, 1)
    with jax.named_scope("ag2"):
        arrived(11, slot(1, 0, 1), tb)
        arrived(13, slot(1, 1, 1), tb)
        arrived(12, slot(2, 0, 1), tb)
        arrived(14, slot(2, 1, 1), tb)
    run(stage_f, 3, 4, 5, 6)
    run(stage_a, 2)
    run(stage_w, 0, 1)
    run(stage_r, 3, 4)
    run(stage_w, 2)
    finish(0)
    finish(1)
    run(stage_a, 3)
    run(stage_r, 5)
    run(stage_a, 4)
    run(stage_w, 3)
    with jax.named_scope("ag3"):
        arrived(5, slot(3, 0, 0), part)
        arrived(6, slot(3, 0, 0) + part, part)
        to_core(6, 3, 0)
        arrived(7, slot(3, 1, 0), part)
        arrived(8, slot(3, 1, 0) + part, part)
        to_core(7, 3, 1)
        arrived(15, slot(3, 0, 1), tb)
        arrived(16, slot(3, 1, 1), tb)
    run(stage_f, 7)
    run(stage_r, 6)
    finish(2)
    run(stage_a, 5)
    run(stage_w, 4)
    finish(3)

    last = chunks - 1

    def step(t, carry):
        def at(lag, fn):
            with jax.named_scope(fn.__name__):
                fn(t - lag)

        def at_end(lag, fn):
            j, b, k = place(t - lag)

            @pl.when(k == 3)
            def _():
                with jax.named_scope(fn.__name__):
                    fn(j)

        at(0, stage_f)
        at(1, stage_r)
        at(2, stage_a)
        at(3, stage_w)
        at(4, stage_dx)
        at(4, stage_dw)

        @pl.when(t >= 14)
        def _():
            at_end(7, stage_g)

        @pl.when(t >= 17)
        def _():
            at_end(10, stage_e)

        return carry

    lax.fori_loop(8, units, step, 0)

    def dx_rows(b, zr, cr):
        return pl.ds(slot(b, zr, cr), tb)

    def core_copy(b):
        return remote(dxs.at[b], dxr.at[b], dxc_s.at[b], dxc_r.at[b], partner)

    def y1_copy(zr):
        return remote(dxs.at[3, zr], ybuf.at[zr], y1_s.at[zr], y1_r.at[zr], (up, down)[zr])

    def y2_copy(way, zr):
        return remote(
            dxs.at[2 - way, zr], y2.at[way, zr], y2_s.at[way, zr], y2_r.at[way, zr],
            (up, down)[way],
        )

    def send_core(b):
        for zr in range(2):
            dxs[b, zr] = dx[dx_rows(b, zr, 1), :].astype(BF16)
        core_copy(b).start()

    def chip_sum(b, zr):
        return dx[dx_rows(b, zr, 0), :] + dxr[b, zr].astype(F32)

    def ring_early(way):
        b, zr = 2 - way, 1 - way
        if way == 0:
            with jax.named_scope("core_wait"):
                core_copy(b).wait()
        dxs[b, zr] = chip_sum(b, zr).astype(BF16)
        y2_copy(way, zr).start()

    def ring_late(way):
        b, zr = 2 - way, way
        if way == 1:
            with jax.named_scope("core_wait"):
                core_copy(b).wait()
        with jax.named_scope("y1_wait"):
            y1_copy(zr).wait_recv()
        dxs[b, zr] = (chip_sum(b, zr) + ybuf[zr].astype(F32)).astype(BF16)
        y2_copy(way, zr).start()

    run(stage_r, units - 1)
    run(stage_a, units - 2)
    run(stage_w, units - 3)
    run(stage_dx, units - 4)
    send_core(3)
    run(stage_a, units - 1)
    run(stage_w, units - 2)
    run(stage_dw, units - 4)
    core_copy(3).wait()
    for zr in range(2):
        dxs[3, zr] = chip_sum(3, zr).astype(BF16)
        y1_copy(zr).start()
    run(stage_dx, units - 3)
    send_core(2)
    run(stage_dw, units - 3)
    run(stage_w, units - 1)
    run(stage_g, last - 1)
    run(stage_dx, units - 2)
    send_core(1)
    ring_early(0)
    run(stage_dw, units - 2)
    ring_late(1)
    run(arrive_dx, units - 1)
    run(stage_dw, units - 1)
    ring_early(1)
    ring_late(0)
    run(add_dx, units - 1)
    send_core(0)
    core_copy(0).wait()
    for zr in range(2):
        dx[dx_rows(0, zr, 0), :] = chip_sum(0, zr)
    z_copy = remote(dxs.at[0, 1], zbuf, z_s.at[0], z_r.at[0], near)
    with jax.named_scope("y2_wait"):
        for way in range(2):
            y2_copy(way, 1).wait_recv()
    total = dx[dx_rows(0, 1, 0), :] + y2[0, 1].astype(F32) + y2[1, 1].astype(F32)
    dxs[0, 1] = total.astype(BF16)
    z_copy.start()
    with jax.named_scope("g_last"):
        stage_g(last)
    with jax.named_scope("y2_wait"):
        for way in range(2):
            y2_copy(way, 0).wait_recv()
    dx[dx_rows(0, 0, 0), :] = (
        dx[dx_rows(0, 0, 0), :] + y2[0, 0].astype(F32) + y2[1, 0].astype(F32)
    )
    run(stage_e, last - 2)
    run(stage_e, last - 1)
    with jax.named_scope("z_wait"):
        z_copy.wait()
    dx_out[...] = dx[dx_rows(0, 0, 0), :] + zbuf[...].astype(F32)
    run(stage_e, last)

    with jax.named_scope("end"):
        for copy in started:
            copy.wait_send()
        for u in range(units - KEEP, units):
            sent(u)
        for u in range(units):
            for way in range(2):
                a1(u, way, x).wait_send()
            a2(u, opp).wait_send()
        for j in range(chunks):
            for k in range(4):
                p1(j, k).wait_send()
                p2(j, k).wait_send()
        for zr in range(2):
            y1_copy(zr).wait_send()
            for way in range(2):
                y2_copy(way, zr).wait_send()


def combine(own, got, dx, dx_out, g_out, u_out, o_out):
    rows = g_out.shape[0]
    where = pl.ds(pl.multiple_of(pl.program_id(0) * rows, rows), rows)
    for j in range(own.shape[0]):
        for m, out in enumerate((g_out, u_out, o_out)):
            lanes = pl.ds(m * W, W)
            total = own[j, where, lanes].astype(F32) + got[j, where, lanes].astype(F32)
            out[:, pl.ds(j * W, W)] = total
    some = dx_out.shape[0]
    dx_out[...] = dx[pl.ds(pl.multiple_of(pl.program_id(0) * some, some), some), :]


def per_device(codes, scales, mask, cot, wg, wu, wo):
    tb, dl = codes.shape
    fl = wg.shape[1]
    chunks = fl // W
    units = 4 * chunks
    dims = (tb, dl, chunks)
    tile = tb + FOOT
    vmem = pl.BlockSpec(memory_space=pltpu.VMEM)
    hbm = pl.BlockSpec(memory_space=pl.ANY)
    dma = pltpu.SemaphoreType.DMA
    grads = pltpu.VMEM((chunks, dl, 3 * W), BF16)
    dx, own, got = pl.pallas_call(
        functools.partial(kernel, dims),
        out_shape=(pltpu.VMEM((tb, dl), F32), grads, grads),
        in_specs=[vmem] * 4 + [hbm] * 3,
        out_specs=(vmem, vmem, vmem),
        scratch_shapes=[
            pltpu.VMEM((16 * tb, 2 * dl), BF16),
            pltpu.VMEM((chunks, dl, 3 * W), BF16),
            pltpu.VMEM((KEEP, 4, tile, 3 * W), jnp.int16),
            pltpu.VMEM((units, tile, 3 * W), jnp.int16),
            pltpu.VMEM((units, 2, tile, 3 * W), jnp.int16),
            pltpu.VMEM((chunks, 16 * tb, 3 * W), BF16),
            pltpu.VMEM((16 * tb, dl), F32),
            pltpu.VMEM((3, dl, 3 * W), F32),
            pltpu.VMEM((chunks, dl, 3 * W), BF16),
            pltpu.VMEM((4, 2, tb, dl), BF16),
            pltpu.VMEM((4, 2, tb, dl), BF16),
            pltpu.VMEM((2, tb, dl), BF16),
            pltpu.VMEM((2, 2, tb, dl), BF16),
            pltpu.VMEM((tb, dl), BF16),
            dma((chunks, 3)),
            dma((17,)), dma((17,)),
            dma((units,)), dma((units,)),
            dma((units, 2)), dma((units, 2)),
            dma((units, 2)), dma((units, 2)),
            dma((units,)), dma((units,)),
            dma((chunks, 4)), dma((chunks, 4)),
            dma((chunks, 4)), dma((chunks, 4)),
            dma((4,)), dma((4,)),
            dma((2,)), dma((2,)),
            dma((2, 2)), dma((2, 2)),
            dma((1,)), dma((1,)),
        ],
        compiler_params=pltpu.CompilerParams(
            collective_id=0, has_side_effects=True, vmem_limit_bytes=57671680
        ),
        name="ffn_backward",
    )(codes, scales.T, mask[None, :], cot, wg, wu, wo)
    weight = jax.ShapeDtypeStruct((dl, fl), F32)
    steps = 8
    rows = dl // steps
    return pl.pallas_call(
        combine,
        grid=(steps,),
        out_shape=(jax.ShapeDtypeStruct((tb, dl), F32), weight, weight, weight),
        in_specs=[vmem] * 3,
        out_specs=[pl.BlockSpec((tb // steps, dl), lambda i: (i, 0))]
        + [pl.BlockSpec((rows, fl), lambda i: (i, 0))] * 3,
        compiler_params=pltpu.CompilerParams(vmem_limit_bytes=24 * 1024 * 1024),
        name="combine",
    )(own, got, dx)


def solution(mesh):
    tokens = P(("dp", "col"), "row")
    weights = P("row", "col")
    return jax.shard_map(
        per_device,
        mesh=mesh,
        in_specs=(tokens, tokens, P(("dp", "col")), tokens, weights, weights, weights),
        out_specs=(tokens, weights, weights, weights),
        check_vma=False,
    )
```

```python
import functools

import jax
import jax.numpy as jnp
from jax import lax
from jax.experimental import pallas as pl
from jax.experimental.pallas import tpu as pltpu
from jax.sharding import PartitionSpec as P

MESH = pl.DeviceIdType.MESH
ROOT = 0.7978845608028654
CUBIC = 0.044715
W = 128
KEEP = 6
FOOT = 8
F32 = jnp.float32
BF16 = jnp.bfloat16


def gelu_pair(values):
    inside = ROOT * (values + CUBIC * values * values * values)
    tangent = jnp.tanh(inside)
    activated = 0.5 * values * (1.0 + tangent)
    derivative = 0.5 * (1.0 + tangent) + 0.5 * values * (1.0 - tangent * tangent) * ROOT * (
        1.0 + 3.0 * CUBIC * values * values
    )
    return activated, derivative


def coded(part):
    most = jnp.maximum(jnp.max(jnp.abs(part), axis=0, keepdims=True), 1e-30)
    power = jnp.floor(jnp.log(most) * 1.4426950408889634) + 1.0
    units = jnp.round(part * jnp.exp2(15.0 - power))
    units = jnp.clip(units, -32767.0, 32767.0).astype(jnp.int32).astype(jnp.int16)
    foot = jnp.broadcast_to(power, (FOOT, part.shape[1])).astype(jnp.int32).astype(jnp.int16)
    return units, foot


def store_coded(tile, lanes, part):
    rows = part.shape[0]
    units, foot = coded(part)
    tile[pl.ds(0, rows), lanes] = units
    tile[pl.ds(rows, FOOT), lanes] = foot


def decoded(tile, rows, lanes):
    power = tile[pl.ds(rows, FOOT), lanes].astype(jnp.int32).astype(F32)[0:1]
    units = tile[pl.ds(0, rows), lanes].astype(jnp.int32).astype(F32)
    return units * jnp.exp2(power - 15.0)


def kernel(
    dims,
    codes, scales, mask, cot, wg, wu, wo,
    dx_out, dws, dwr,
    sl, wc, pb, r1, r2, guh, dx, acc, relay, dxs, dxr, ybuf, y2, zbuf,
    w_sem, ag_s, ag_r, rs1_s, rs1_r, rs2_s, rs2_r, a1_s, a1_r, a2_s, a2_r,
    p1_s, p1_r, p2_s, p2_r, dxc_s, dxc_r, y1_s, y1_r, y2_s, y2_r, z_s, z_r,
):
    tb, dl, chunks = dims
    blk = 4 * tb
    units = 4 * chunks
    x = lax.axis_index("row")
    col = lax.axis_index("col")
    dp = lax.axis_index("dp")
    core = lax.rem(col, 2)
    y = lax.rem(col // 2, 4)
    z = col // 8
    opp = lax.rem(x + 2, 4)

    def at_col(dz, dy, dc):
        zz = (1 - z) if dz else z
        cc = (1 - core) if dc else core
        return {"col": (zz * 4 + lax.rem(y + dy, 4)) * 2 + cc}

    def beside(way):
        return lax.rem(x + 1 + 2 * way, 4)

    def to_row(way):
        return {"row": beside(way)}

    partner = at_col(0, 0, 1)
    up, down = at_col(0, 1, 0), at_col(0, 3, 0)
    near = at_col(1, 0, 0)
    far = dict(near, dp=1 - dp)

    barrier = pltpu.get_barrier_semaphore()
    peers = [to_row(0), to_row(1), partner, up, down, near, far]
    for peer in peers:
        pl.semaphore_signal(barrier, inc=1, device_id=peer, device_id_type=MESH)

    def weight_copy(j, m, src):
        return pltpu.make_async_copy(
            src.at[:, pl.ds(j * W, W)], wc.at[j, :, pl.ds(m * W, W)], w_sem.at[j, m]
        )

    for j in range(chunks):
        for m, src in enumerate((wg, wu, wo)):
            weight_copy(j, m, src).start()

    nb = scales.shape[0]
    flat = jnp.concatenate(
        [scales[...].astype(F32), jnp.broadcast_to(mask[...], (8, tb)).astype(F32),
         jnp.zeros((128 - nb - 8, tb), F32)], axis=0,
    )
    tall = jnp.transpose(flat)
    for k in range(nb):
        lanes = pl.ds(k * 128, 128)
        level = (2 * codes[:, lanes] - 3).astype(F32) * tall[:, k : k + 1]
        sl[pl.ds(0, tb), lanes] = (level * 0.0625).astype(BF16)
        live = cot[:, lanes].astype(F32) * tall[:, nb : nb + 1]
        sl[pl.ds(0, tb), pl.ds(dl + k * 128, 128)] = live.astype(BF16)

    with jax.named_scope("barrier"):
        pl.semaphore_wait(barrier, len(peers))

    def remote(src, dst, s_sem, r_sem, device):
        return pltpu.make_async_remote_copy(
            src_ref=src, dst_ref=dst, send_sem=s_sem, recv_sem=r_sem,
            device_id=device, device_id_type=MESH,
        )

    def slot(b, zr, cr):
        return (b * 4 + zr * 2 + cr) * tb

    def rows(start, count):
        return sl.at[pl.ds(start, count)]

    started = []

    def gather(kind, src, dst, count, device):
        copy = remote(rows(src, count), rows(dst, count), ag_s.at[kind], ag_r.at[kind], device)
        copy.start()
        started.append(copy)

    def arrived(kind, dst, count):
        remote(rows(dst, count), rows(dst, count), ag_s.at[kind], ag_r.at[kind], partner).wait_recv()

    def to_core(kind, b, zr):
        gather(9 + kind, slot(b, zr, 0), slot(b, zr, 1), tb, partner)

    part = tb // 2
    gather(0, slot(0, 0, 0), slot(0, 1, 0), tb, near)
    gather(1, slot(0, 0, 0), slot(1, 0, 0), tb, up)
    gather(2, slot(0, 0, 0), slot(2, 0, 0), tb, down)
    to_core(0, 0, 0)
    for j in range(chunks):
        for m, src in enumerate((wg, wu, wo)):
            weight_copy(j, m, src).wait()

    def place(u):
        if isinstance(u, int) and u < 3:
            return u, 0, 0
        late, whole = (u + 3) // 12, u // 12
        first = (u - 3) // 2 + 1
        k = lax.rem(u, 4)
        return (
            (1 - late) * lax.rem(u - 3, 2) + late * (u // 4),
            (1 - late) * first + late * (4 - whole - k),
            (1 - late) * first + late * k,
        )

    def unit(u):
        return place(u)[:2]

    def held(u):
        return pb.at[lax.rem(u, KEEP)]

    def grad_rows(j, b, owner):
        return guh.at[j, pl.ds(pl.multiple_of((b * 4 + owner) * tb, tb), tb)]

    def rs1(u, way):
        return remote(held(u).at[opp], r1.at[u], rs1_s.at[u], rs1_r.at[u], to_row(way))

    def rs2(u, way):
        return remote(
            held(u).at[beside(way)], r2.at[u, way], rs2_s.at[u, way], rs2_r.at[u, way], to_row(way)
        )

    def a1(u, way, owner):
        j, b = unit(u)
        ref = grad_rows(j, b, owner)
        return remote(ref, ref, a1_s.at[u, way], a1_r.at[u, way], to_row(way))

    def a2(u, owner):
        j, b = unit(u)
        ref = grad_rows(j, b, owner)
        return remote(ref, ref, a2_s.at[u], a2_r.at[u], to_row(lax.rem(u, 2)))

    def sent(u):
        rs1(u, lax.rem(u, 2)).wait_send()
        for way in range(2):
            rs2(u, way).wait_send()

    def stage_f(u):
        j, b = unit(u)
        if isinstance(u, int):
            if u >= KEEP:
                sent(u - KEEP)
        else:
            sent(u - KEEP)
        where = pl.ds(pl.multiple_of(b * blk, blk), blk)
        both = jnp.dot(
            sl[where, pl.ds(0, dl)], wc[j, :, pl.ds(0, 2 * W)], preferred_element_type=F32
        )
        back = jnp.dot(
            sl[where, pl.ds(dl, dl)], wc[j, :, pl.ds(2 * W, W)], preferred_element_type=F32
        )
        for o in range(4):
            tile = held(u).at[o]
            store_coded(tile, pl.ds(0, 2 * W), both[o * tb : (o + 1) * tb])
            store_coded(tile, pl.ds(2 * W, W), back[o * tb : (o + 1) * tb])
        rs1(u, lax.rem(u, 2)).start()

    def stage_r(u):
        j, b = unit(u)
        way = lax.rem(u, 2)
        rs2(u, 1 - way).start()
        with jax.named_scope("r_wait"):
            rs1(u, way).wait_recv()
        tile = held(u).at[beside(way)]
        for m in range(3):
            lanes = pl.ds(m * W, W)
            total = decoded(tile, tb, lanes) + decoded(r1.at[u], tb, lanes)
            store_coded(tile, lanes, total)
        rs2(u, way).start()

    def stage_a(u):
        j, b = unit(u)
        with jax.named_scope("a_wait"):
            for way in range(2):
                rs2(u, way).wait_recv()
        tiles = (held(u).at[x], r2.at[u, 0], r2.at[u, 1])
        powers = [
            [
                jnp.exp2(t[pl.ds(tb, FOOT), pl.ds(m * W, W)].astype(jnp.int32).astype(F32)[0:1] - 15.0)
                for t in tiles
            ]
            for m in range(3)
        ]
        step = tb // 2

        def body(k, carry):
            some = pl.ds(pl.multiple_of(k * step, step), step)
            sums = []
            for m in range(3):
                total = None
                for t, power in zip(tiles, powers[m]):
                    term = t[some, pl.ds(m * W, W)].astype(jnp.int32).astype(F32) * power
                    total = term if total is None else total + term
                sums.append(total)
            gate, up_part, back = sums
            activated, derivative = gelu_pair(gate)
            to = pl.ds(pl.multiple_of((b * 4 + x) * tb + k * step, step), step)
            guh[j, to, pl.ds(0, W)] = (back * up_part * derivative).astype(BF16)
            guh[j, to, pl.ds(W, W)] = (back * activated).astype(BF16)
            guh[j, to, pl.ds(2 * W, W)] = (activated * up_part).astype(BF16)
            return carry

        lax.fori_loop(0, 2, body, 0)
        for way in range(2):
            a1(u, way, x).start()

    def stage_w(u):
        way = lax.rem(u, 2)
        with jax.named_scope("w_wait"):
            a1(u, way, beside(1 - way)).wait_recv()
        a2(u, beside(1 - way)).start()

    def arrive_dx(u):
        j, b = unit(u)
        way = lax.rem(u, 2)
        with jax.named_scope("b_wait"):
            a1(u, 1 - way, beside(way)).wait_recv()
            a2(u, opp).wait_recv()

    def add_dx(u):
        j, b = unit(u)
        where = pl.ds(pl.multiple_of(b * blk, blk), blk)
        more = lax.dot_general(
            guh[j, where, pl.ds(0, 2 * W)], wc[j, :, pl.ds(0, 2 * W)],
            (((1,), (1,)), ((), ())), preferred_element_type=F32,
        )
        dx[where, :] = dx[where, :] + more

    def stage_dx(u):
        arrive_dx(u)
        add_dx(u)

    quarter = dl // 4

    def to_z(other):
        return dict(near, dp=dp + other * (1 - 2 * dp))

    def piece(k):
        return pl.ds(pl.multiple_of(k * quarter, quarter), quarter)

    def p1(j, k):
        return remote(
            dws.at[j, piece(k)], relay.at[j, piece(k)], p1_s.at[j, k], p1_r.at[j, k], to_z(k // 2)
        )

    def p2(j, k):
        return remote(
            relay.at[j, piece(k)], dwr.at[j, piece(k)], p2_s.at[j, k], p2_r.at[j, k],
            to_z(1 - k // 2),
        )

    def stage_dw(u):
        j, b, k = place(u)
        where = pl.ds(pl.multiple_of(b * blk, blk), blk)
        sums = acc.at[lax.rem(j, 3)]

        def body(i, carry):
            q = lax.rem(i, 2) * 2 + i // 2
            some = lax.dot_general(
                sl[where, piece(q)], guh[j, where, pl.ds(0, 2 * W)],
                (((0,), (0,)), ((), ())), preferred_element_type=F32,
            )
            more = lax.dot_general(
                sl[where, pl.ds(pl.multiple_of(dl + q * quarter, quarter), quarter)],
                guh[j, where, pl.ds(2 * W, W)],
                (((0,), (0,)), ((), ())), preferred_element_type=F32,
            )
            sums[piece(q), pl.ds(0, 2 * W)] = sums[piece(q), pl.ds(0, 2 * W)] + some
            sums[piece(q), pl.ds(2 * W, W)] = sums[piece(q), pl.ds(2 * W, W)] + more

            @pl.when(k == 3)
            def _():
                dws[j, piece(q), :] = sums[piece(q), :].astype(BF16)
                sums[piece(q), :] = jnp.zeros((quarter, 3 * W), F32)
                p1(j, q).start()

            return carry

        lax.fori_loop(0, 4, body, 0)

    def stage_g(j):
        for k in (0, 2, 1, 3):
            with jax.named_scope("g_wait"):
                p1(j, k).wait_recv()
            p2(j, k).start()

    def stage_e(j):
        with jax.named_scope("e_wait"):
            for k in (0, 2, 1, 3):
                p2(j, k).wait_recv()

    dx[...] = jnp.zeros_like(dx)
    acc[...] = jnp.zeros_like(acc)

    arrived(0, slot(0, 1, 0), tb)
    gather(3, slot(0, 1, 0), slot(1, 1, 0), tb, up)
    gather(4, slot(0, 1, 0), slot(2, 1, 0), tb, down)
    to_core(1, 0, 1)
    arrived(1, slot(1, 0, 0), tb)
    gather(5, slot(1, 0, 0), slot(3, 0, 0), part, up)
    to_core(2, 1, 0)
    arrived(2, slot(2, 0, 0), tb)
    gather(6, slot(2, 0, 0) + part, slot(3, 0, 0) + part, part, down)
    to_core(3, 2, 0)
    arrived(9, slot(0, 0, 1), tb)
    arrived(10, slot(0, 1, 1), tb)

    def run(stage, *which):
        for u in which:
            with jax.named_scope(f"{stage.__name__}_{u}"):
                stage(u)

    def finish(u):
        run(stage_dx, u)
        run(stage_dw, u)

    run(stage_f, 0, 1, 2)
    run(stage_r, 0, 1, 2)
    run(stage_a, 0)
    with jax.named_scope("ag1"):
        arrived(3, slot(1, 1, 0), tb)
        gather(7, slot(1, 1, 0), slot(3, 1, 0), part, up)
        to_core(4, 1, 1)
        arrived(4, slot(2, 1, 0), tb)
        gather(8, slot(2, 1, 0) + part, slot(3, 1, 0) + part, part, down)
        to_core(5, 2, 1)
    run(stage_a, 1)
    with jax.named_scope("ag2"):
        arrived(11, slot(1, 0, 1), tb)
        arrived(13, slot(1, 1, 1), tb)
        arrived(12, slot(2, 0, 1), tb)
        arrived(14, slot(2, 1, 1), tb)
    run(stage_f, 3, 4, 5, 6)
    run(stage_a, 2)
    run(stage_w, 0, 1)
    run(stage_r, 3, 4)
    run(stage_w, 2)
    finish(0)
    finish(1)
    run(stage_a, 3)
    run(stage_r, 5)
    run(stage_a, 4)
    run(stage_w, 3)
    with jax.named_scope("ag3"):
        arrived(5, slot(3, 0, 0), part)
        arrived(6, slot(3, 0, 0) + part, part)
        to_core(6, 3, 0)
        arrived(7, slot(3, 1, 0), part)
        arrived(8, slot(3, 1, 0) + part, part)
        to_core(7, 3, 1)
        arrived(15, slot(3, 0, 1), tb)
        arrived(16, slot(3, 1, 1), tb)
    run(stage_f, 7)
    run(stage_r, 6)
    finish(2)
    run(stage_a, 5)
    run(stage_w, 4)
    finish(3)

    last = chunks - 1

    def step(t, carry):
        def at(lag, fn):
            with jax.named_scope(fn.__name__):
                fn(t - lag)

        def at_end(lag, fn):
            j, b, k = place(t - lag)

            @pl.when(k == 3)
            def _():
                with jax.named_scope(fn.__name__):
                    fn(j)

        at(0, stage_f)
        at(1, stage_r)
        at(2, stage_a)
        at(3, stage_w)
        at(4, stage_dx)
        at(4, stage_dw)

        @pl.when(t >= 14)
        def _():
            at_end(7, stage_g)

        return carry

    lax.fori_loop(8, units, step, 0)

    def dx_rows(b, zr, cr):
        return pl.ds(slot(b, zr, cr), tb)

    def core_copy(b):
        return remote(dxs.at[b], dxr.at[b], dxc_s.at[b], dxc_r.at[b], partner)

    def y1_copy(zr):
        return remote(dxs.at[3, zr], ybuf.at[zr], y1_s.at[zr], y1_r.at[zr], (up, down)[zr])

    def y2_copy(way, zr):
        return remote(
            dxs.at[2 - way, zr], y2.at[way, zr], y2_s.at[way, zr], y2_r.at[way, zr],
            (up, down)[way],
        )

    def send_core(b):
        for zr in range(2):
            dxs[b, zr] = dx[dx_rows(b, zr, 1), :].astype(BF16)
        core_copy(b).start()

    def chip_sum(b, zr):
        return dx[dx_rows(b, zr, 0), :] + dxr[b, zr].astype(F32)

    def ring_early(way):
        b, zr = 2 - way, 1 - way
        if way == 0:
            with jax.named_scope("core_wait"):
                core_copy(b).wait()
        dxs[b, zr] = chip_sum(b, zr).astype(BF16)
        y2_copy(way, zr).start()

    def ring_late(way):
        b, zr = 2 - way, way
        if way == 1:
            with jax.named_scope("core_wait"):
                core_copy(b).wait()
        with jax.named_scope("y1_wait"):
            y1_copy(zr).wait_recv()
        dxs[b, zr] = (chip_sum(b, zr) + ybuf[zr].astype(F32)).astype(BF16)
        y2_copy(way, zr).start()

    run(stage_r, units - 1)
    run(stage_a, units - 2)
    run(stage_w, units - 3)
    run(stage_dx, units - 4)
    send_core(3)
    run(stage_a, units - 1)
    run(stage_w, units - 2)
    run(stage_dw, units - 4)
    core_copy(3).wait()
    for zr in range(2):
        dxs[3, zr] = chip_sum(3, zr).astype(BF16)
        y1_copy(zr).start()
    run(stage_dx, units - 3)
    send_core(2)
    run(stage_dw, units - 3)
    run(stage_w, units - 1)
    run(stage_g, last - 1)
    run(stage_dx, units - 2)
    send_core(1)
    ring_early(0)
    run(stage_dw, units - 2)
    run(arrive_dx, units - 1)
    run(stage_dw, units - 1)
    ring_late(1)
    ring_early(1)
    ring_late(0)
    run(add_dx, units - 1)
    send_core(0)
    core_copy(0).wait()
    for zr in range(2):
        dx[dx_rows(0, zr, 0), :] = chip_sum(0, zr)
    z_copy = remote(dxs.at[0, 1], zbuf, z_s.at[0], z_r.at[0], near)
    with jax.named_scope("y2_wait"):
        for way in range(2):
            y2_copy(way, 1).wait_recv()
    total = dx[dx_rows(0, 1, 0), :] + y2[0, 1].astype(F32) + y2[1, 1].astype(F32)
    dxs[0, 1] = total.astype(BF16)
    z_copy.start()
    with jax.named_scope("g_last"):
        stage_g(last)
    with jax.named_scope("y2_wait"):
        for way in range(2):
            y2_copy(way, 0).wait_recv()
    dx[dx_rows(0, 0, 0), :] = (
        dx[dx_rows(0, 0, 0), :] + y2[0, 0].astype(F32) + y2[1, 0].astype(F32)
    )
    for j in range(last):
        run(stage_e, j)
    with jax.named_scope("z_wait"):
        z_copy.wait()
    dx_out[...] = dx[dx_rows(0, 0, 0), :] + zbuf[...].astype(F32)
    run(stage_e, last)

    with jax.named_scope("end"):
        for copy in started:
            copy.wait_send()
        for u in range(units - KEEP, units):
            sent(u)
        for u in range(units):
            for way in range(2):
                a1(u, way, x).wait_send()
            a2(u, opp).wait_send()
        for j in range(chunks):
            for k in range(4):
                p1(j, k).wait_send()
                p2(j, k).wait_send()
        for zr in range(2):
            y1_copy(zr).wait_send()
            for way in range(2):
                y2_copy(way, zr).wait_send()


def combine(own, got, dx, dx_out, g_out, u_out, o_out):
    rows = g_out.shape[0]
    where = pl.ds(pl.multiple_of(pl.program_id(0) * rows, rows), rows)
    for j in range(own.shape[0]):
        for m, out in enumerate((g_out, u_out, o_out)):
            lanes = pl.ds(m * W, W)
            total = own[j, where, lanes].astype(F32) + got[j, where, lanes].astype(F32)
            out[:, pl.ds(j * W, W)] = total
    some = dx_out.shape[0]
    dx_out[...] = dx[pl.ds(pl.multiple_of(pl.program_id(0) * some, some), some), :]


def per_device(codes, scales, mask, cot, wg, wu, wo):
    tb, dl = codes.shape
    fl = wg.shape[1]
    chunks = fl // W
    units = 4 * chunks
    dims = (tb, dl, chunks)
    tile = tb + FOOT
    vmem = pl.BlockSpec(memory_space=pltpu.VMEM)
    hbm = pl.BlockSpec(memory_space=pl.ANY)
    dma = pltpu.SemaphoreType.DMA
    grads = pltpu.VMEM((chunks, dl, 3 * W), BF16)
    dx, own, got = pl.pallas_call(
        functools.partial(kernel, dims),
        out_shape=(pltpu.VMEM((tb, dl), F32), grads, grads),
        in_specs=[vmem] * 4 + [hbm] * 3,
        out_specs=(vmem, vmem, vmem),
        scratch_shapes=[
            pltpu.VMEM((16 * tb, 2 * dl), BF16),
            pltpu.VMEM((chunks, dl, 3 * W), BF16),
            pltpu.VMEM((KEEP, 4, tile, 3 * W), jnp.int16),
            pltpu.VMEM((units, tile, 3 * W), jnp.int16),
            pltpu.VMEM((units, 2, tile, 3 * W), jnp.int16),
            pltpu.VMEM((chunks, 16 * tb, 3 * W), BF16),
            pltpu.VMEM((16 * tb, dl), F32),
            pltpu.VMEM((3, dl, 3 * W), F32),
            pltpu.VMEM((chunks, dl, 3 * W), BF16),
            pltpu.VMEM((4, 2, tb, dl), BF16),
            pltpu.VMEM((4, 2, tb, dl), BF16),
            pltpu.VMEM((2, tb, dl), BF16),
            pltpu.VMEM((2, 2, tb, dl), BF16),
            pltpu.VMEM((tb, dl), BF16),
            dma((chunks, 3)),
            dma((17,)), dma((17,)),
            dma((units,)), dma((units,)),
            dma((units, 2)), dma((units, 2)),
            dma((units, 2)), dma((units, 2)),
            dma((units,)), dma((units,)),
            dma((chunks, 4)), dma((chunks, 4)),
            dma((chunks, 4)), dma((chunks, 4)),
            dma((4,)), dma((4,)),
            dma((2,)), dma((2,)),
            dma((2, 2)), dma((2, 2)),
            dma((1,)), dma((1,)),
        ],
        compiler_params=pltpu.CompilerParams(
            collective_id=0, has_side_effects=True, vmem_limit_bytes=57671680
        ),
        name="ffn_backward",
    )(codes, scales.T, mask[None, :], cot, wg, wu, wo)
    weight = jax.ShapeDtypeStruct((dl, fl), F32)
    steps = 8
    rows = dl // steps
    return pl.pallas_call(
        combine,
        grid=(steps,),
        out_shape=(jax.ShapeDtypeStruct((tb, dl), F32), weight, weight, weight),
        in_specs=[vmem] * 3,
        out_specs=[pl.BlockSpec((tb // steps, dl), lambda i: (i, 0))]
        + [pl.BlockSpec((rows, fl), lambda i: (i, 0))] * 3,
        compiler_params=pltpu.CompilerParams(vmem_limit_bytes=24 * 1024 * 1024),
        name="combine",
    )(own, got, dx)


def solution(mesh):
    tokens = P(("dp", "col"), "row")
    weights = P("row", "col")
    return jax.shard_map(
        per_device,
        mesh=mesh,
        in_specs=(tokens, tokens, P(("dp", "col")), tokens, weights, weights, weights),
        out_specs=(tokens, weights, weights, weights),
        check_vma=False,
    )
```
